32 devices in a mesh: section: 4 (over z), dp: 4 (over y, x), mp: 2 (over core).
Axes of the slice: x: 2, y: 2, z: 4, core: 2. Of those that a mesh axis runs over, the one named last changes fastest.
Arguments:
- fwd_in: bfloat16 [4, 2048, 1024], P('section', ('dp', 'mp')), may hold values from -6 to 6
- stash: bfloat16 [4, 2048, 1024], P('section', ('dp', 'mp')), may hold values from -6 to 6
- cot: bfloat16 [4, 2048, 1024], P('section', ('dp', 'mp')), may hold values from -8 to 8
- w_in: bfloat16 [4, 2048, 1024], P('section', 'mp'), may hold values from -0.1875 to 0.1875
- w_out: bfloat16 [4, 2048, 1024], P('section', 'mp'), may hold values from -0.125 to 0.125
- gain: float32 [4, 1024], P('section'), may hold values from 0.1 to 1.9
Outputs:
- passed_fwd: bfloat16 [4, 2048, 1024], P('section', ('dp', 'mp'))
- passed_grad: bfloat16 [4, 2048, 1024], P('section', ('dp', 'mp'))
- grad_w_in: bfloat16 [4, 2048, 1024], P('section', 'mp', 'dp')
- grad_w_out: bfloat16 [4, 2048, 1024], P('section', 'mp', 'dp')
The draws below stay inside these ranges and needn't reach their ends.
All inputs are finite; a program needn't handle non-finite values.
Results may differ from the reference program's by a relative error of at most 0.015.
Values may be sent and summed in bfloat16 or wider, within the bound.
A program may use at most 64 MiB of HBM per device.

```python
import jax
import jax.numpy as jnp
from jax import lax

D = 1024
HID = 2048
TOK = 512
HID_DEV = 1024
TOKENS = 2048
SECTIONS = 4
N_DP = 4
N_MP = 2


def raised(array, rng, source, target, blocks, factor):
    def block_of(axis_at):
        return (jnp.arange(array.shape[axis_at]) // (array.shape[axis_at] // blocks)).reshape((-1,) + (1,) * (array.ndim - 1 - axis_at))

    one_side = jax.random.permutation(rng, blocks)[block_of(target)]
    other_side = (block_of(target) + blocks // 2) % blocks
    return jnp.where((block_of(source) == one_side) | (block_of(source) == other_side), factor * array, array)


def steps_of(own_key, shape, split, least, high):
    level, own = 1.0, jax.random.fold_in(own_key, 6)
    for position, blocks in split:
        steps = jnp.exp(jax.random.uniform(jax.random.fold_in(own, position), (blocks,), jnp.float32, least / len(split), high / len(split)))
        level = level * jnp.repeat(steps, shape[position] // blocks).reshape([-1 if axis == position else 1 for axis in range(len(shape))])
    return level


def gaussian(key, shape, width, reach, pieces=(), dtype=jnp.bfloat16):
    result = width * jax.random.normal(key, shape, jnp.float32)
    if pieces:
        result = result * steps_of(key, shape, pieces, -0.22, 0.18)
    return jnp.clip(result, -reach, reach).astype(dtype)


def heavy_noise(rng, dims, deviation, most, pieces, heavy, held_as=jnp.bfloat16):
    entries = deviation * jax.random.normal(rng, dims, jnp.float32)
    if pieces:
        entries = entries * steps_of(rng, dims, pieces, -0.22, 0.18)
    return jnp.clip(raised(entries, jax.random.fold_in(rng, 3), *heavy), -most, most).astype(held_as)


def setup_inputs(seed: int = 0) -> dict:
    streams_of = jax.random.split(jax.random.key(seed), 7)
    fwd_in = gaussian(streams_of[0], (SECTIONS, TOKENS, D), 1.0, 6.0, ((0, 4), (1, 8)))
    stash = gaussian(streams_of[1], (SECTIONS, TOKENS, D), 1.0, 6.0, ((0, 4), (1, 8)))
    cot = heavy_noise(streams_of[2], (SECTIONS, TOKENS, D), 1.0, 8.0, ((0, 4), (1, 8)), (1, 2, 8, 2.0))
    w_in = gaussian(streams_of[3], (SECTIONS, HID, D), D ** -0.5, 0.1875, ((0, 4), (1, 2)))
    w_out = gaussian(streams_of[4], (SECTIONS, HID, D), HID ** -0.5, 0.125, ((0, 4), (1, 2)))
    gain = jnp.clip(1.0 + 0.18 * jax.random.normal(streams_of[5], (SECTIONS, D), jnp.float32), 0.1, 1.9)
    return {"fwd_in": fwd_in, "stash": stash, "cot": cot, "w_in": w_in, "w_out": w_out, "gain": gain}


norm_eps = 1e-05
gelu_coef = 0.7978845608

def gelu_value(v):
    inner = jnp.tanh(gelu_coef * (v + 0.044715 * v * v * v))
    return 0.5 * v * (1.0 + inner)

def gelu_slope(v):
    inner = jnp.tanh(gelu_coef * (v + 0.044715 * v * v * v))
    return 0.5 * (1.0 + inner) + 0.5 * v * (1.0 - inner * inner) * gelu_coef * (1.0 + 0.134145 * v * v)

def prepare(x, w_in, gain):
    xf = x.astype(jnp.float32)
    scale = lax.rsqrt(lax.optimization_barrier(jnp.mean(xf * xf, axis=-1, keepdims=True)) + norm_eps)
    normed = (xf * scale * gain[None, :]).astype(jnp.bfloat16)
    pre = lax.dot_general(normed, w_in, (((1,), (1,)), ((), ())), preferred_element_type=jnp.float32)
    act = gelu_value(pre).astype(jnp.bfloat16)
    return (xf, scale, normed, pre, act)

def group_sum(left, right):
    rows = left.shape[0]
    lhs = left.reshape(rows, N_MP, HID_DEV).astype(jnp.float32)
    rhs = right.reshape(N_MP, HID_DEV, right.shape[1]).astype(jnp.float32)
    parts = jnp.einsum('tgh,ghd->gtd', lhs, rhs).astype(jnp.bfloat16)
    parts = lax.optimization_barrier(parts)
    return lax.optimization_barrier(jnp.sum(parts.astype(jnp.float32), axis=0))

def replica_sum(left, right):
    lhs = left.reshape(N_DP, TOK, left.shape[1]).astype(jnp.float32)
    rhs = right.reshape(N_DP, TOK, right.shape[1]).astype(jnp.float32)
    parts = jnp.einsum('rth,rtd->rhd', lhs, rhs).astype(jnp.bfloat16)
    parts = lax.optimization_barrier(parts)
    return lax.optimization_barrier(jnp.sum(parts.astype(jnp.float32), axis=0)).astype(jnp.bfloat16)

def reference(fwd_in, stash, cot, w_in, w_out, gain):
    outs = []
    grads = []
    g_ins = []
    g_outs = []
    for section in range(SECTIONS):
        xf, scale, normed, pre, act = prepare(fwd_in[section], w_in[section], gain[section])
        outs.append((xf + group_sum(act, w_out[section])).astype(jnp.bfloat16))
        sf, sscale, snormed, spre, sact = prepare(stash[section], w_in[section], gain[section])
        cot_rows = cot[section]
        d_act = lax.dot_general(cot_rows, w_out[section], (((1,), (1,)), ((), ())), preferred_element_type=jnp.float32)
        d_pre = (d_act * gelu_slope(spre)).astype(jnp.bfloat16)
        d_norm = group_sum(d_pre, w_in[section])
        push = d_norm * gain[section][None, :]
        mixed = lax.optimization_barrier(jnp.mean(sf * push, axis=-1, keepdims=True))
        dx = cot_rows.astype(jnp.float32) + sscale * push - sf * sscale * sscale * sscale * mixed
        grads.append(dx.astype(jnp.bfloat16))
        g_outs.append(replica_sum(sact, cot_rows))
        g_ins.append(replica_sum(d_pre, snormed))
    passed_fwd = jnp.roll(jnp.stack(outs), 1, axis=0)
    passed_grad = jnp.roll(jnp.stack(grads), -1, axis=0)
    return (passed_fwd, passed_grad, jnp.stack(g_ins), jnp.stack(g_outs))
```

```python
import jax
import jax.numpy as jnp
from jax import lax
from jax.experimental import pallas as pl
from jax.experimental.pallas import tpu as pltpu
from jax.sharding import PartitionSpec as P

norm_eps = 1e-05
gelu_coef = 0.7978845608


def shifted(x, axis, by):
    length = lax.axis_size(axis)
    return lax.ppermute(x, axis, [(i, (i + by) % length) for i in range(length)])


def gelu_value(v):
    inner = jnp.tanh(gelu_coef * (v + 0.044715 * v * v * v))
    return 0.5 * v * (1.0 + inner)


def gelu_slope(v):
    inner = jnp.tanh(gelu_coef * (v + 0.044715 * v * v * v))
    return 0.5 * (1.0 + inner) + 0.5 * v * (1.0 - inner * inner) * gelu_coef * (
        1.0 + 0.134145 * v * v
    )


def prepare(x, w_first, gain_row):
    xf = x.astype(jnp.float32)
    scale = lax.rsqrt(jnp.mean(xf * xf, axis=-1, keepdims=True) + norm_eps)
    normed = (xf * scale * gain_row[None, :]).astype(jnp.bfloat16)
    pre = lax.dot_general(
        normed, w_first, (((1,), (1,)), ((), ())), preferred_element_type=jnp.float32
    )
    act = gelu_value(pre).astype(jnp.bfloat16)
    return (scale, normed, pre, act)


def on_device(fwd_in, stash, cot, w_in, w_out, gain):
    x_fwd = fwd_in[0]
    x_bwd = stash[0]
    cot_local = cot[0]
    w_first = w_in[0]
    w_second = w_out[0]
    gain_row = gain[0]
    local_rows = x_fwd.shape[0]
    scale, normed, pre, act = prepare(
        lax.all_gather(x_fwd, "mp", axis=0, tiled=True), w_first, gain_row
    )
    terms = jnp.dot(act, w_second, preferred_element_type=jnp.float32)
    branch = lax.psum_scatter(
        terms.astype(jnp.bfloat16), "mp", scatter_dimension=0, tiled=True
    ).astype(jnp.float32)
    out = (x_fwd.astype(jnp.float32) + branch).astype(jnp.bfloat16)
    passed_fwd = shifted(out, "section", 1)
    rows_x, rows_cot = (
        lax.all_gather(x_bwd, "mp", axis=0, tiled=True),
        lax.all_gather(cot_local, "mp", axis=0, tiled=True),
    )
    scale, normed, pre, act = prepare(rows_x, w_first, gain_row)
    d_act = lax.dot_general(
        rows_cot, w_second, (((1,), (1,)), ((), ())), preferred_element_type=jnp.float32
    )
    d_pre = (d_act * gelu_slope(pre)).astype(jnp.bfloat16)
    d_norm = lax.psum_scatter(
        jnp.dot(d_pre, w_first, preferred_element_type=jnp.float32).astype(jnp.bfloat16),
        "mp",
        scatter_dimension=0,
        tiled=True,
    ).astype(jnp.float32)
    offset = lax.axis_index("mp") * local_rows
    own_scale = lax.dynamic_slice_in_dim(scale, offset, local_rows, 0)
    shard_x = x_bwd.astype(jnp.float32)
    push = d_norm * gain_row[None, :]
    mixed = jnp.mean(shard_x * push, axis=-1, keepdims=True)
    dx = (
        cot_local.astype(jnp.float32)
        + own_scale * push
        - shard_x * own_scale * own_scale * own_scale * mixed
    )
    passed_grad = shifted(dx.astype(jnp.bfloat16), "section", -1)
    term_out = lax.dot_general(
        act, rows_cot, (((0,), (0,)), ((), ())), preferred_element_type=jnp.float32
    )
    term_in = lax.dot_general(
        d_pre, normed, (((0,), (0,)), ((), ())), preferred_element_type=jnp.float32
    )
    sum_in, sum_out = (
        lax.psum_scatter(
            term_in.astype(jnp.bfloat16), "dp", scatter_dimension=1, tiled=True
        ).astype(jnp.float32),
        lax.psum_scatter(
            term_out.astype(jnp.bfloat16), "dp", scatter_dimension=1, tiled=True
        ).astype(jnp.float32),
    )
    return (
        passed_fwd[None],
        passed_grad[None],
        sum_in.astype(jnp.bfloat16)[None],
        sum_out.astype(jnp.bfloat16)[None],
    )


MESH = pl.DeviceIdType.MESH
vmem_bytes = 67_043_328
NT = (((1,), (1,)), ((), ()))
TN = (((0,), (0,)), ((), ()))
OUT, IN = range(2)
pieces = 2


def tile_of(total, most):
    size = min(total, most)
    while total % size:
        size //= 2
    return size


def remote(src, dst, send, recv, target):
    return pltpu.make_async_remote_copy(
        src_ref=src, dst_ref=dst, send_sem=send, recv_sem=recv,
        device_id=target, device_id_type=MESH,
    )


def start_remote(src, dst, send, recv, target):
    copy = remote(src, dst, send, recv, target)
    copy.start()
    return copy


def write_kernel(a, b, c, d, a_out, b_out, c_out, d_out, sems):
    copies = [
        pltpu.make_async_copy(src, dst, sems.at[i])
        for i, (src, dst) in enumerate(((a, a_out), (b, b_out), (c, c_out), (d, d_out)))
    ]
    for copy in copies:
        copy.start()
    for copy in copies:
        copy.wait()


def relay_kernel(
    fwd_hbm, stash_hbm, cot_hbm, win_hbm, wout_hbm, gain_hbm,
    pass_fwd, pass_grad, gin_ref, gout_ref,
    gain_ref, xf, xs, xc, win, wout,
    nf, nb, slope, act_t, dpre_t, act, own_sum, parts, landed,
    mp_out, mp_in, own_terms, z_out,
    load_sem, swap_send, swap_recv, ag_send, ag_recv,
    mp_send, mp_recv, rs_send, rs_recv, z_send, z_recv,
):
    rows = pass_fwd.shape[0]
    tokens = 2 * rows
    hid, width = win.shape
    cols = gin_ref.shape[1]
    n_sec = lax.axis_size("section")
    sec, dp, mp = lax.axis_index("section"), lax.axis_index("dp"), lax.axis_index("mp")
    y, x = lax.div(dp, 2), lax.rem(dp, 2)
    flip_x, flip_y = y * 2 + (1 - x), (1 - y) * 2 + x
    across = (1 - y) * 2 + (1 - x)
    peer = {"mp": 1 - mp}
    after, before = {"section": lax.rem(sec + 1, n_sec)}, {"section": lax.rem(sec + n_sec - 1, n_sec)}
    partner = mp * flip_x + (1 - mp) * flip_y

    barrier = pltpu.get_barrier_semaphore()
    greeted = [after, before, peer] + [
        {"dp": chip, "mp": core} for chip in (flip_x, flip_y) for core in (mp, 1 - mp)
    ]
    for target in greeted:
        pl.semaphore_signal(barrier, inc=1, device_id=target, device_id_type=MESH)

    own, other = pl.ds(0, rows), pl.ds(rows, rows)
    near, far = pl.ds(0, tokens), pl.ds(tokens, tokens)
    local = (
        (gain_hbm, gain_ref), (fwd_hbm, xf.at[own]), (win_hbm, win), (wout_hbm, wout),
        (stash_hbm, xs.at[own]), (cot_hbm, xc.at[own]),
    )
    loads = [
        pltpu.make_async_copy(src, dst, load_sem.at[i]) for i, (src, dst) in enumerate(local)
    ]
    for load in loads:
        load.start()
    load_gain, load_fwd, load_win, load_wout, load_stash, load_cot = loads
    pl.semaphore_wait(barrier, len(greeted))

    swap_fwd = start_remote(fwd_hbm, xf.at[other], swap_send.at[0], swap_recv.at[0], peer)

    def column(block):
        return pl.ds(pl.multiple_of(block * cols, cols), cols)

    targets = (
        ({"dp": flip_x, "mp": 0}, (across, flip_x, dp, flip_y)),
        ({"dp": flip_y, "mp": 1}, (across, flip_y, dp, flip_x)),
    )
    slot = pl.ds(pl.multiple_of(tokens + mp * rows, rows), rows)
    gathers = []
    for d, (target, _) in enumerate(targets):
        gathers.append(
            start_remote(stash_hbm, xs.at[slot], ag_send.at[d, 0], ag_recv.at[mp, 0], target)
        )
    swap_stash = start_remote(stash_hbm, xs.at[other], swap_send.at[1], swap_recv.at[1], peer)
    swap_cot = start_remote(cot_hbm, xc.at[other], swap_send.at[2], swap_recv.at[2], peer)
    for i in range(4):
        for d, (target, order) in enumerate(targets):
            at = column(order[i])
            gathers.append(
                start_remote(
                    cot_hbm.at[:, at], xc.at[slot, at],
                    ag_send.at[d, 1 + i], ag_recv.at[mp, 1 + i], target,
                )
            )

    gathered = (partner, dp, (1 - mp) * flip_x + mp * flip_y, across)

    def await_gather(i):
        for core in range(2):
            rows_at = pl.ds(tokens + core * rows, rows)
            if i == 0:
                src, dst = stash_hbm, xs.at[rows_at]
            else:
                at = column(gathered[i - 1])
                src, dst = cot_hbm.at[:, at], xc.at[rows_at, at]
            remote(src, dst, ag_send.at[0, i], ag_recv.at[core, i], peer).wait_recv()

    step = tile_of(rows, 64)

    def normalise(source, target, first, count):
        def body(i, carry):
            at = pl.ds(pl.multiple_of(first + i * step, step), step)
            v = source[at, :].astype(jnp.float32)
            r = lax.rsqrt(jnp.mean(v * v, axis=-1, keepdims=True) + norm_eps)
            target[at, :] = (v * r * gain_ref[...]).astype(jnp.bfloat16)
            return carry

        lax.fori_loop(0, count // step, body, 0)

    block = tile_of(hid, 256)

    def backward_pre(span):
        def body(i, carry):
            at = pl.ds(pl.multiple_of(i * block, block), block)
            v = lax.dot_general(
                win[at, :], nb[span, :], NT, preferred_element_type=jnp.float32
            )
            square = v * v
            t = jnp.tanh(gelu_coef * (v + 0.044715 * square * v))
            act_t[at, span] = (0.5 * v * (1.0 + t)).astype(jnp.bfloat16)
            slope[at, :] = 0.5 * (1.0 + t) + 0.5 * v * (1.0 - t * t) * gelu_coef * (
                1.0 + 0.134145 * square
            )
            return carry

        lax.fori_loop(0, hid // block, body, 0)

    def backward_slope(span):
        def body(i, carry):
            at = pl.ds(pl.multiple_of(i * block, block), block)
            d_act = lax.dot_general(
                wout[at, :], xc[span, :], NT, preferred_element_type=jnp.float32
            )
            dpre_t[at, span] = (d_act * slope[at, :]).astype(jnp.bfloat16)
            return carry

        lax.fori_loop(0, hid // block, body, 0)

    def forward(span):
        def body(i, carry):
            at = pl.ds(pl.multiple_of(i * block, block), block)
            v = lax.dot_general(
                nf[span, :], win[at, :], NT, preferred_element_type=jnp.float32
            )
            t = jnp.tanh(gelu_coef * (v + 0.044715 * v * v * v))
            act[:, at] = (0.5 * v * (1.0 + t)).astype(jnp.bfloat16)
            return carry

        lax.fori_loop(0, hid // block, body, 0)
        return jnp.dot(
            act[...], wout[...], preferred_element_type=jnp.float32
        ).astype(jnp.bfloat16)

    load_gain.wait()
    load_fwd.wait()
    normalise(xf, nf, 0, rows)
    load_win.wait()
    load_wout.wait()
    swap_fwd.wait_recv()
    normalise(xf, nf, rows, rows)
    mp_out[1] = forward(other)
    swap_branch = start_remote(mp_out.at[1], mp_in.at[1], mp_send.at[1], mp_recv.at[1], peer)
    own_terms[1] = forward(own)
    swap_branch.wait_recv()

    def finish_forward(i, carry):
        at = pl.ds(pl.multiple_of(i * step, step), step)
        branch = own_terms[1, at, :].astype(jnp.float32) + mp_in[1, at, :].astype(jnp.float32)
        z_out[1, at, :] = (xf[at, :].astype(jnp.float32) + branch).astype(jnp.bfloat16)
        return carry

    lax.fori_loop(0, rows // step, finish_forward, 0)
    relay_fwd = start_remote(z_out.at[1], pass_fwd, z_send.at[1], z_recv.at[1], after)

    load_stash.wait()
    swap_stash.wait_recv()
    normalise(xs, nb, 0, tokens)
    backward_pre(near)
    load_cot.wait()
    swap_cot.wait_recv()
    backward_slope(near)

    def d_norm(span):
        return lax.dot_general(
            dpre_t[:, span], win[...], TN, preferred_element_type=jnp.float32
        ).astype(jnp.bfloat16)

    mp_out[0] = d_norm(other)
    swap_grad = start_remote(mp_out.at[0], mp_in.at[0], mp_send.at[0], mp_recv.at[0], peer)
    own_terms[0] = d_norm(own)
    swap_grad.wait_recv()

    def finish_grad(i, carry):
        at = pl.ds(pl.multiple_of(i * step, step), step)
        v = xs[at, :].astype(jnp.float32)
        r = lax.rsqrt(jnp.mean(v * v, axis=-1, keepdims=True) + norm_eps)
        push = (
            own_terms[0, at, :].astype(jnp.float32) + mp_in[0, at, :].astype(jnp.float32)
        ) * gain_ref[...]
        mixed = jnp.mean(v * push, axis=-1, keepdims=True)
        dx = xc[at, :].astype(jnp.float32) + r * push - v * (r * r * r * mixed)
        z_out[0, at, :] = dx.astype(jnp.bfloat16)
        return carry

    lax.fori_loop(0, rows // step, finish_grad, 0)
    relay_grad = start_remote(z_out.at[0], pass_grad, z_send.at[0], z_recv.at[0], before)

    operands = {OUT: (act_t, xc), IN: (dpre_t, nb)}
    size = hid // pieces
    bands = [pl.ds(p * size, size) for p in range(pieces)]
    sent = {}

    def product(g, p, owner):
        left, right = operands[g]
        return jnp.dot(
            left[bands[p], :], right[:, column(owner)], preferred_element_type=jnp.float32
        )

    def give(g):
        for p in range(pieces):
            parts[g, bands[p], :] = product(g, p, partner).astype(jnp.bfloat16)
            sent[g, p] = start_remote(
                parts.at[g, bands[p]], landed.at[g, bands[p]],
                rs_send.at[g, p], rs_recv.at[g, p], {"dp": partner},
            )

    def keep(g):
        for p in range(pieces):
            own_sum[g, bands[p], :] = product(g, p, dp)

    await_gather(0)
    normalise(xs, nb, tokens, tokens)
    backward_pre(far)
    await_gather(1)
    give(OUT)
    await_gather(2)
    keep(OUT)
    await_gather(3)
    await_gather(4)
    backward_slope(far)
    give(IN)
    keep(IN)

    for g, result in ((OUT, gout_ref), (IN, gin_ref)):
        for p in range(pieces):
            sent[g, p].wait_recv()
            result[bands[p], :] = (
                own_sum[g, bands[p], :] + landed[g, bands[p], :].astype(jnp.float32)
            ).astype(jnp.bfloat16)

    relay_grad.wait_recv()
    relay_fwd.wait_recv()
    for copy in [
        swap_fwd, swap_stash, swap_cot, *gathers, swap_grad, swap_branch,
        relay_grad, relay_fwd, *sent.values(),
    ]:
        copy.wait_send()


def relay_on_device(fwd_in, stash, cot, w_in, w_out, gain):
    rows, width = stash.shape[1:]
    hid = w_in.shape[1]
    tokens = rows * lax.axis_size("mp")
    cols = width // lax.axis_size("dp")
    bf16 = jnp.bfloat16
    vmem = pl.BlockSpec(memory_space=pltpu.VMEM)
    hbm = pl.BlockSpec(memory_space=pl.ANY)
    dma = pltpu.SemaphoreType.DMA
    held = (rows * width + hid * cols) * 2 * jnp.dtype(bf16).itemsize
    results = pl.pallas_call(
        relay_kernel,
        out_shape=(pltpu.VMEM((rows, width), bf16),) * 2 + (pltpu.VMEM((hid, cols), bf16),) * 2,
        in_specs=[hbm] * 6,
        out_specs=(vmem,) * 4,
        scratch_shapes=[
            pltpu.VMEM((1, width), jnp.float32),
            pltpu.VMEM((tokens, width), bf16),
            pltpu.VMEM((2 * tokens, width), bf16),
            pltpu.VMEM((2 * tokens, width), bf16),
            pltpu.VMEM((hid, width), bf16),
            pltpu.VMEM((hid, width), bf16),
            pltpu.VMEM((tokens, width), bf16),
            pltpu.VMEM((2 * tokens, width), bf16),
            pltpu.VMEM((hid, tokens), jnp.float32),
            pltpu.VMEM((hid, 2 * tokens), bf16),
            pltpu.VMEM((hid, 2 * tokens), bf16),
            pltpu.VMEM((rows, hid), bf16),
            pltpu.VMEM((2, hid, cols), jnp.float32),
            pltpu.VMEM((2, hid, cols), bf16),
            pltpu.VMEM((2, hid, cols), bf16),
            pltpu.VMEM((2, rows, width), bf16),
            pltpu.VMEM((2, rows, width), bf16),
            pltpu.VMEM((2, rows, width), bf16),
            pltpu.VMEM((2, rows, width), bf16),
            dma((6,)),
            dma((3,)),
            dma((3,)),
            dma((2, 5)),
            dma((2, 5)),
            dma((2,)),
            dma((2,)),
            dma((2, pieces)),
            dma((2, pieces)),
            dma((2,)),
            dma((2,)),
        ],
        compiler_params=pltpu.CompilerParams(
            collective_id=0, has_side_effects=True,
            vmem_limit_bytes=vmem_bytes - held - 2**17,
        ),
    )(fwd_in[0], stash[0], cot[0], w_in[0], w_out[0], gain)
    results = pl.pallas_call(
        write_kernel,
        out_shape=tuple(jax.ShapeDtypeStruct(r.shape, r.dtype) for r in results),
        in_specs=[vmem] * 4,
        out_specs=(hbm,) * 4,
        scratch_shapes=[dma((4,))],
        compiler_params=pltpu.CompilerParams(vmem_limit_bytes=4 * 2**20),
    )(*results)
    return tuple(r[None] for r in results)


def fits_relay(mesh):
    return mesh.shape["dp"] == 4 and mesh.shape["mp"] == 2 and mesh.shape["section"] > 1


def solution(mesh):
    in_specs = (
        P("section", ("dp", "mp"), None),
        P("section", ("dp", "mp"), None),
        P("section", ("dp", "mp"), None),
        P("section", "mp", None),
        P("section", "mp", None),
        P("section", None),
    )
    out_specs = (
        P("section", ("dp", "mp"), None),
        P("section", ("dp", "mp"), None),
        P("section", "mp", "dp"),
        P("section", "mp", "dp"),
    )
    return jax.shard_map(
        relay_on_device if fits_relay(mesh) else on_device,
        mesh=mesh,
        in_specs=in_specs,
        out_specs=out_specs,
        check_vma=False,
    )
```

```python
import jax
import jax.numpy as jnp
from jax import lax
from jax.experimental import pallas as pl
from jax.experimental.pallas import tpu as pltpu
from jax.sharding import PartitionSpec as P

norm_eps = 1e-05
gelu_coef = 0.7978845608


def shifted(x, axis, by):
    length = lax.axis_size(axis)
    return lax.ppermute(x, axis, [(i, (i + by) % length) for i in range(length)])


def gelu_value(v):
    inner = jnp.tanh(gelu_coef * (v + 0.044715 * v * v * v))
    return 0.5 * v * (1.0 + inner)


def gelu_slope(v):
    inner = jnp.tanh(gelu_coef * (v + 0.044715 * v * v * v))
    return 0.5 * (1.0 + inner) + 0.5 * v * (1.0 - inner * inner) * gelu_coef * (
        1.0 + 0.134145 * v * v
    )


def prepare(x, w_first, gain_row):
    xf = x.astype(jnp.float32)
    scale = lax.rsqrt(jnp.mean(xf * xf, axis=-1, keepdims=True) + norm_eps)
    normed = (xf * scale * gain_row[None, :]).astype(jnp.bfloat16)
    pre = lax.dot_general(
        normed, w_first, (((1,), (1,)), ((), ())), preferred_element_type=jnp.float32
    )
    act = gelu_value(pre).astype(jnp.bfloat16)
    return (scale, normed, pre, act)


def on_device(fwd_in, stash, cot, w_in, w_out, gain):
    x_fwd = fwd_in[0]
    x_bwd = stash[0]
    cot_local = cot[0]
    w_first = w_in[0]
    w_second = w_out[0]
    gain_row = gain[0]
    local_rows = x_fwd.shape[0]
    scale, normed, pre, act = prepare(
        lax.all_gather(x_fwd, "mp", axis=0, tiled=True), w_first, gain_row
    )
    terms = jnp.dot(act, w_second, preferred_element_type=jnp.float32)
    branch = lax.psum_scatter(
        terms.astype(jnp.bfloat16), "mp", scatter_dimension=0, tiled=True
    ).astype(jnp.float32)
    out = (x_fwd.astype(jnp.float32) + branch).astype(jnp.bfloat16)
    passed_fwd = shifted(out, "section", 1)
    rows_x, rows_cot = (
        lax.all_gather(x_bwd, "mp", axis=0, tiled=True),
        lax.all_gather(cot_local, "mp", axis=0, tiled=True),
    )
    scale, normed, pre, act = prepare(rows_x, w_first, gain_row)
    d_act = lax.dot_general(
        rows_cot, w_second, (((1,), (1,)), ((), ())), preferred_element_type=jnp.float32
    )
    d_pre = (d_act * gelu_slope(pre)).astype(jnp.bfloat16)
    d_norm = lax.psum_scatter(
        jnp.dot(d_pre, w_first, preferred_element_type=jnp.float32).astype(jnp.bfloat16),
        "mp",
        scatter_dimension=0,
        tiled=True,
    ).astype(jnp.float32)
    offset = lax.axis_index("mp") * local_rows
    own_scale = lax.dynamic_slice_in_dim(scale, offset, local_rows, 0)
    shard_x = x_bwd.astype(jnp.float32)
    push = d_norm * gain_row[None, :]
    mixed = jnp.mean(shard_x * push, axis=-1, keepdims=True)
    dx = (
        cot_local.astype(jnp.float32)
        + own_scale * push
        - shard_x * own_scale * own_scale * own_scale * mixed
    )
    passed_grad = shifted(dx.astype(jnp.bfloat16), "section", -1)
    term_out = lax.dot_general(
        act, rows_cot, (((0,), (0,)), ((), ())), preferred_element_type=jnp.float32
    )
    term_in = lax.dot_general(
        d_pre, normed, (((0,), (0,)), ((), ())), preferred_element_type=jnp.float32
    )
    sum_in, sum_out = (
        lax.psum_scatter(
            term_in.astype(jnp.bfloat16), "dp", scatter_dimension=1, tiled=True
        ).astype(jnp.float32),
        lax.psum_scatter(
            term_out.astype(jnp.bfloat16), "dp", scatter_dimension=1, tiled=True
        ).astype(jnp.float32),
    )
    return (
        passed_fwd[None],
        passed_grad[None],
        sum_in.astype(jnp.bfloat16)[None],
        sum_out.astype(jnp.bfloat16)[None],
    )


MESH = pl.DeviceIdType.MESH
vmem_bytes = 67_043_328
NT = (((1,), (1,)), ((), ()))
TN = (((0,), (0,)), ((), ()))
OUT, IN = range(2)
pieces = 2


def tile_of(total, most):
    size = min(total, most)
    while total % size:
        size //= 2
    return size


def remote(src, dst, send, recv, target):
    return pltpu.make_async_remote_copy(
        src_ref=src, dst_ref=dst, send_sem=send, recv_sem=recv,
        device_id=target, device_id_type=MESH,
    )


def start_remote(src, dst, send, recv, target):
    copy = remote(src, dst, send, recv, target)
    copy.start()
    return copy


def write_kernel(a, b, c, d, a_out, b_out, c_out, d_out, sems):
    copies = [
        pltpu.make_async_copy(src, dst, sems.at[i])
        for i, (src, dst) in enumerate(((a, a_out), (b, b_out), (c, c_out), (d, d_out)))
    ]
    for copy in copies:
        copy.start()
    for copy in copies:
        copy.wait()


def relay_kernel(
    fwd_hbm, stash_hbm, cot_hbm, win_hbm, wout_hbm, gain_hbm,
    pass_fwd, pass_grad, gin_ref, gout_ref,
    gain_ref, xf, xs, xc, win, wout,
    nf, nb, slope, act_t, dpre_t, act, own_sum, parts, landed,
    mp_out, mp_in, own_terms, z_out,
    load_sem, swap_send, swap_recv, ag_send, ag_recv,
    mp_send, mp_recv, rs_send, rs_recv, z_send, z_recv, above, below, wrapped,
):
    rows = pass_fwd.shape[0]
    tokens = 2 * rows
    hid, width = win.shape
    cols = gin_ref.shape[1]
    n_sec = lax.axis_size("section")
    sec, dp, mp = lax.axis_index("section"), lax.axis_index("dp"), lax.axis_index("mp")
    y, x = lax.div(dp, 2), lax.rem(dp, 2)
    flip_x, flip_y = y * 2 + (1 - x), (1 - y) * 2 + x
    across = (1 - y) * 2 + (1 - x)
    peer = {"mp": 1 - mp}
    after, before = {"section": lax.rem(sec + 1, n_sec)}, {"section": lax.rem(sec + n_sec - 1, n_sec)}
    partner = mp * flip_x + (1 - mp) * flip_y

    barrier = pltpu.get_barrier_semaphore()
    greeted = [peer] + [
        {"dp": chip, "mp": core} for chip in (flip_x, flip_y) for core in (mp, 1 - mp)
    ]

    def signal(sem, target):
        pl.semaphore_signal(sem, inc=1, device_id=target, device_id_type=MESH)

    for target in greeted:
        signal(barrier, target)

    @pl.when(sec < n_sec - 1)
    def _():
        signal(barrier, after)

    own, other = pl.ds(0, rows), pl.ds(rows, rows)
    near, far = pl.ds(0, tokens), pl.ds(tokens, tokens)
    local = (
        (stash_hbm, xs.at[own]), (cot_hbm, xc.at[own]), (fwd_hbm, xf.at[own]),
        (gain_hbm, gain_ref), (win_hbm, win), (wout_hbm, wout),
    )
    loads = [
        pltpu.make_async_copy(src, dst, load_sem.at[i]) for i, (src, dst) in enumerate(local)
    ]
    for load in loads:
        load.start()
    load_stash, load_cot, load_fwd, load_gain, load_win, load_wout = loads
    pl.semaphore_wait(barrier, len(greeted) + jnp.minimum(sec, 1))
    load_stash.wait()

    def column(block):
        return pl.ds(pl.multiple_of(block * cols, cols), cols)

    targets = (
        ({"dp": flip_x, "mp": 0}, (across, flip_x, dp, flip_y)),
        ({"dp": flip_y, "mp": 1}, (across, flip_y, dp, flip_x)),
    )
    slot = pl.ds(pl.multiple_of(tokens + mp * rows, rows), rows)
    gathers = []
    for d, (target, _) in enumerate(targets):
        gathers.append(
            start_remote(xs.at[own], xs.at[slot], ag_send.at[d, 0], ag_recv.at[mp, 0], target)
        )
    load_fwd.wait()
    swap_fwd = start_remote(xf.at[own], xf.at[other], swap_send.at[0], swap_recv.at[0], peer)
    load_cot.wait()
    swap_stash = start_remote(xs.at[own], xs.at[other], swap_send.at[1], swap_recv.at[1], peer)
    swap_cot = start_remote(xc.at[own], xc.at[other], swap_send.at[2], swap_recv.at[2], peer)
    for i in range(4):
        for d, (target, order) in enumerate(targets):
            at = column(order[i])
            gathers.append(
                start_remote(
                    xc.at[own, at], xc.at[slot, at],
                    ag_send.at[d, 1 + i], ag_recv.at[mp, 1 + i], target,
                )
            )

    @pl.when(sec > 0)
    def _():
        signal(above, before)

    @pl.when((sec == 1) & (sec < n_sec - 1))
    def _():
        pl.semaphore_wait(above, 1)
        signal(below, after)

    gathered = (partner, dp, (1 - mp) * flip_x + mp * flip_y, across)

    def await_gather(i):
        for core in range(2):
            rows_at = pl.ds(tokens + core * rows, rows)
            if i == 0:
                src, dst = xs.at[own], xs.at[rows_at]
            else:
                at = column(gathered[i - 1])
                src, dst = xc.at[own, at], xc.at[rows_at, at]
            remote(src, dst, ag_send.at[0, i], ag_recv.at[core, i], peer).wait_recv()

    step = tile_of(rows, 64)

    def normalise(source, target, first, count):
        def body(i, carry):
            at = pl.ds(pl.multiple_of(first + i * step, step), step)
            v = source[at, :].astype(jnp.float32)
            r = lax.rsqrt(jnp.mean(v * v, axis=-1, keepdims=True) + norm_eps)
            target[at, :] = (v * r * gain_ref[...]).astype(jnp.bfloat16)
            return carry

        lax.fori_loop(0, count // step, body, 0)

    block = tile_of(hid, 256)

    def backward_pre(span):
        def body(i, carry):
            at = pl.ds(pl.multiple_of(i * block, block), block)
            v = lax.dot_general(
                win[at, :], nb[span, :], NT, preferred_element_type=jnp.float32
            )
            square = v * v
            t = jnp.tanh(gelu_coef * (v + 0.044715 * square * v))
            act_t[at, span] = (0.5 * v * (1.0 + t)).astype(jnp.bfloat16)
            slope[at, :] = 0.5 * (1.0 + t) + 0.5 * v * (1.0 - t * t) * gelu_coef * (
                1.0 + 0.134145 * square
            )
            return carry

        lax.fori_loop(0, hid // block, body, 0)

    def backward_slope(span):
        def body(i, carry):
            at = pl.ds(pl.multiple_of(i * block, block), block)
            d_act = lax.dot_general(
                wout[at, :], xc[span, :], NT, preferred_element_type=jnp.float32
            )
            dpre_t[at, span] = (d_act * slope[at, :]).astype(jnp.bfloat16)
            return carry

        lax.fori_loop(0, hid // block, body, 0)

    def forward(span):
        def body(i, carry):
            at = pl.ds(pl.multiple_of(i * block, block), block)
            v = lax.dot_general(
                nf[span, :], win[at, :], NT, preferred_element_type=jnp.float32
            )
            t = jnp.tanh(gelu_coef * (v + 0.044715 * v * v * v))
            act[:, at] = (0.5 * v * (1.0 + t)).astype(jnp.bfloat16)
            return carry

        lax.fori_loop(0, hid // block, body, 0)
        return jnp.dot(
            act[...], wout[...], preferred_element_type=jnp.float32
        ).astype(jnp.bfloat16)

    load_gain.wait()
    normalise(xf, nf, 0, rows)
    load_win.wait()
    load_wout.wait()
    swap_fwd.wait_recv()
    normalise(xf, nf, rows, rows)
    mp_out[1] = forward(other)
    swap_branch = start_remote(mp_out.at[1], mp_in.at[1], mp_send.at[1], mp_recv.at[1], peer)

    @pl.when((sec > 1) & (sec < n_sec - 1))
    def _():
        pl.semaphore_wait(above, 1)
        pl.semaphore_wait(below, 1)
        signal(below, after)

    own_terms[1] = forward(own)
    swap_branch.wait_recv()

    def finish_forward(i, carry):
        at = pl.ds(pl.multiple_of(i * step, step), step)
        branch = own_terms[1, at, :].astype(jnp.float32) + mp_in[1, at, :].astype(jnp.float32)
        z_out[1, at, :] = (xf[at, :].astype(jnp.float32) + branch).astype(jnp.bfloat16)
        return carry

    lax.fori_loop(0, rows // step, finish_forward, 0)

    @pl.when(sec == 0)
    def _():
        pl.semaphore_wait(above, 1)

    if n_sec > 2:
        @pl.when(sec == n_sec - 1)
        def _():
            pl.semaphore_wait(below, 1)

    @pl.when(sec == n_sec - 1)
    def _():
        signal(wrapped, after)

    relay_fwd = start_remote(z_out.at[1], pass_fwd, z_send.at[1], z_recv.at[1], after)

    swap_stash.wait_recv()
    normalise(xs, nb, 0, tokens)
    backward_pre(near)
    swap_cot.wait_recv()
    backward_slope(near)

    def d_norm(span):
        return lax.dot_general(
            dpre_t[:, span], win[...], TN, preferred_element_type=jnp.float32
        ).astype(jnp.bfloat16)

    mp_out[0] = d_norm(other)
    swap_grad = start_remote(mp_out.at[0], mp_in.at[0], mp_send.at[0], mp_recv.at[0], peer)
    own_terms[0] = d_norm(own)
    swap_grad.wait_recv()

    def finish_grad(i, carry):
        at = pl.ds(pl.multiple_of(i * step, step), step)
        v = xs[at, :].astype(jnp.float32)
        r = lax.rsqrt(jnp.mean(v * v, axis=-1, keepdims=True) + norm_eps)
        push = (
            own_terms[0, at, :].astype(jnp.float32) + mp_in[0, at, :].astype(jnp.float32)
        ) * gain_ref[...]
        mixed = jnp.mean(v * push, axis=-1, keepdims=True)
        dx = xc[at, :].astype(jnp.float32) + r * push - v * (r * r * r * mixed)
        z_out[0, at, :] = dx.astype(jnp.bfloat16)
        return carry

    lax.fori_loop(0, rows // step, finish_grad, 0)

    @pl.when(sec == 0)
    def _():
        pl.semaphore_wait(wrapped, 1)

    relay_grad = start_remote(z_out.at[0], pass_grad, z_send.at[0], z_recv.at[0], before)

    operands = {OUT: (act_t, xc), IN: (dpre_t, nb)}
    size = hid // pieces
    bands = [pl.ds(p * size, size) for p in range(pieces)]
    sent = {}

    def product(g, p, owner):
        left, right = operands[g]
        return jnp.dot(
            left[bands[p], :], right[:, column(owner)], preferred_element_type=jnp.float32
        )

    def give(g):
        for p in range(pieces):
            parts[g, bands[p], :] = product(g, p, partner).astype(jnp.bfloat16)
            sent[g, p] = start_remote(
                parts.at[g, bands[p]], landed.at[g, bands[p]],
                rs_send.at[g, p], rs_recv.at[g, p], {"dp": partner},
            )

    def keep(g):
        for p in range(pieces):
            own_sum[g, bands[p], :] = product(g, p, dp)

    await_gather(0)
    normalise(xs, nb, tokens, tokens)
    backward_pre(far)
    await_gather(1)
    give(OUT)
    await_gather(2)
    keep(OUT)
    await_gather(3)
    await_gather(4)
    backward_slope(far)
    give(IN)
    keep(IN)

    for g, result in ((OUT, gout_ref), (IN, gin_ref)):
        for p in range(pieces):
            sent[g, p].wait_recv()
            result[bands[p], :] = (
                own_sum[g, bands[p], :] + landed[g, bands[p], :].astype(jnp.float32)
            ).astype(jnp.bfloat16)

    relay_grad.wait_recv()
    relay_fwd.wait_recv()
    for copy in [
        swap_fwd, swap_stash, swap_cot, *gathers, swap_grad, swap_branch,
        relay_grad, relay_fwd, *sent.values(),
    ]:
        copy.wait_send()


def relay_on_device(fwd_in, stash, cot, w_in, w_out, gain):
    rows, width = stash.shape[1:]
    hid = w_in.shape[1]
    tokens = rows * lax.axis_size("mp")
    cols = width // lax.axis_size("dp")
    bf16 = jnp.bfloat16
    vmem = pl.BlockSpec(memory_space=pltpu.VMEM)
    hbm = pl.BlockSpec(memory_space=pl.ANY)
    dma = pltpu.SemaphoreType.DMA
    held = (rows * width + hid * cols) * 2 * jnp.dtype(bf16).itemsize
    results = pl.pallas_call(
        relay_kernel,
        out_shape=(pltpu.VMEM((rows, width), bf16),) * 2 + (pltpu.VMEM((hid, cols), bf16),) * 2,
        in_specs=[hbm] * 6,
        out_specs=(vmem,) * 4,
        scratch_shapes=[
            pltpu.VMEM((1, width), jnp.float32),
            pltpu.VMEM((tokens, width), bf16),
            pltpu.VMEM((2 * tokens, width), bf16),
            pltpu.VMEM((2 * tokens, width), bf16),
            pltpu.VMEM((hid, width), bf16),
            pltpu.VMEM((hid, width), bf16),
            pltpu.VMEM((tokens, width), bf16),
            pltpu.VMEM((2 * tokens, width), bf16),
            pltpu.VMEM((hid, tokens), jnp.float32),
            pltpu.VMEM((hid, 2 * tokens), bf16),
            pltpu.VMEM((hid, 2 * tokens), bf16),
            pltpu.VMEM((rows, hid), bf16),
            pltpu.VMEM((2, hid, cols), jnp.float32),
            pltpu.VMEM((2, hid, cols), bf16),
            pltpu.VMEM((2, hid, cols), bf16),
            pltpu.VMEM((2, rows, width), bf16),
            pltpu.VMEM((2, rows, width), bf16),
            pltpu.VMEM((2, rows, width), bf16),
            pltpu.VMEM((2, rows, width), bf16),
            dma((6,)),
            dma((3,)),
            dma((3,)),
            dma((2, 5)),
            dma((2, 5)),
            dma((2,)),
            dma((2,)),
            dma((2, pieces)),
            dma((2, pieces)),
            dma((2,)),
            dma((2,)),
            *[pltpu.SemaphoreType.REGULAR] * 3,
        ],
        compiler_params=pltpu.CompilerParams(
            collective_id=0, has_side_effects=True,
            vmem_limit_bytes=vmem_bytes - held - 2**17,
        ),
    )(fwd_in[0], stash[0], cot[0], w_in[0], w_out[0], gain)
    results = pl.pallas_call(
        write_kernel,
        out_shape=tuple(jax.ShapeDtypeStruct(r.shape, r.dtype) for r in results),
        in_specs=[vmem] * 4,
        out_specs=(hbm,) * 4,
        scratch_shapes=[dma((4,))],
        compiler_params=pltpu.CompilerParams(vmem_limit_bytes=4 * 2**20),
    )(*results)
    return tuple(r[None] for r in results)


def fits_relay(mesh):
    return mesh.shape["dp"] == 4 and mesh.shape["mp"] == 2 and mesh.shape["section"] > 1


def solution(mesh):
    in_specs = (
        P("section", ("dp", "mp"), None),
        P("section", ("dp", "mp"), None),
        P("section", ("dp", "mp"), None),
        P("section", "mp", None),
        P("section", "mp", None),
        P("section", None),
    )
    out_specs = (
        P("section", ("dp", "mp"), None),
        P("section", ("dp", "mp"), None),
        P("section", "mp", "dp"),
        P("section", "mp", "dp"),
    )
    return jax.shard_map(
        relay_on_device if fits_relay(mesh) else on_device,
        mesh=mesh,
        in_specs=in_specs,
        out_specs=out_specs,
        check_vma=False,
    )
```

```python
import jax
import jax.numpy as jnp
from jax import lax
from jax.experimental import pallas as pl
from jax.experimental.pallas import tpu as pltpu
from jax.sharding import PartitionSpec as P

norm_eps = 1e-05
gelu_coef = 0.7978845608


def shifted(x, axis, by):
    length = lax.axis_size(axis)
    return lax.ppermute(x, axis, [(i, (i + by) % length) for i in range(length)])


def gelu_value(v):
    inner = jnp.tanh(gelu_coef * (v + 0.044715 * v * v * v))
    return 0.5 * v * (1.0 + inner)


def gelu_slope(v):
    inner = jnp.tanh(gelu_coef * (v + 0.044715 * v * v * v))
    return 0.5 * (1.0 + inner) + 0.5 * v * (1.0 - inner * inner) * gelu_coef * (
        1.0 + 0.134145 * v * v
    )


def prepare(x, w_first, gain_row):
    xf = x.astype(jnp.float32)
    scale = lax.rsqrt(jnp.mean(xf * xf, axis=-1, keepdims=True) + norm_eps)
    normed = (xf * scale * gain_row[None, :]).astype(jnp.bfloat16)
    pre = lax.dot_general(
        normed, w_first, (((1,), (1,)), ((), ())), preferred_element_type=jnp.float32
    )
    act = gelu_value(pre).astype(jnp.bfloat16)
    return (scale, normed, pre, act)


def on_device(fwd_in, stash, cot, w_in, w_out, gain):
    x_fwd = fwd_in[0]
    x_bwd = stash[0]
    cot_local = cot[0]
    w_first = w_in[0]
    w_second = w_out[0]
    gain_row = gain[0]
    local_rows = x_fwd.shape[0]
    scale, normed, pre, act = prepare(
        lax.all_gather(x_fwd, "mp", axis=0, tiled=True), w_first, gain_row
    )
    terms = jnp.dot(act, w_second, preferred_element_type=jnp.float32)
    branch = lax.psum_scatter(
        terms.astype(jnp.bfloat16), "mp", scatter_dimension=0, tiled=True
    ).astype(jnp.float32)
    out = (x_fwd.astype(jnp.float32) + branch).astype(jnp.bfloat16)
    passed_fwd = shifted(out, "section", 1)
    rows_x, rows_cot = (
        lax.all_gather(x_bwd, "mp", axis=0, tiled=True),
        lax.all_gather(cot_local, "mp", axis=0, tiled=True),
    )
    scale, normed, pre, act = prepare(rows_x, w_first, gain_row)
    d_act = lax.dot_general(
        rows_cot, w_second, (((1,), (1,)), ((), ())), preferred_element_type=jnp.float32
    )
    d_pre = (d_act * gelu_slope(pre)).astype(jnp.bfloat16)
    d_norm = lax.psum_scatter(
        jnp.dot(d_pre, w_first, preferred_element_type=jnp.float32).astype(jnp.bfloat16),
        "mp",
        scatter_dimension=0,
        tiled=True,
    ).astype(jnp.float32)
    offset = lax.axis_index("mp") * local_rows
    own_scale = lax.dynamic_slice_in_dim(scale, offset, local_rows, 0)
    shard_x = x_bwd.astype(jnp.float32)
    push = d_norm * gain_row[None, :]
    mixed = jnp.mean(shard_x * push, axis=-1, keepdims=True)
    dx = (
        cot_local.astype(jnp.float32)
        + own_scale * push
        - shard_x * own_scale * own_scale * own_scale * mixed
    )
    passed_grad = shifted(dx.astype(jnp.bfloat16), "section", -1)
    term_out = lax.dot_general(
        act, rows_cot, (((0,), (0,)), ((), ())), preferred_element_type=jnp.float32
    )
    term_in = lax.dot_general(
        d_pre, normed, (((0,), (0,)), ((), ())), preferred_element_type=jnp.float32
    )
    sum_in, sum_out = (
        lax.psum_scatter(
            term_in.astype(jnp.bfloat16), "dp", scatter_dimension=1, tiled=True
        ).astype(jnp.float32),
        lax.psum_scatter(
            term_out.astype(jnp.bfloat16), "dp", scatter_dimension=1, tiled=True
        ).astype(jnp.float32),
    )
    return (
        passed_fwd[None],
        passed_grad[None],
        sum_in.astype(jnp.bfloat16)[None],
        sum_out.astype(jnp.bfloat16)[None],
    )


MESH = pl.DeviceIdType.MESH
vmem_bytes = 67_043_328
NT = (((1,), (1,)), ((), ()))
TN = (((0,), (0,)), ((), ()))
OUT, IN = range(2)
pieces = 4


def tile_of(total, most):
    size = min(total, most)
    while total % size:
        size //= 2
    return size


def remote(src, dst, send, recv, target):
    return pltpu.make_async_remote_copy(
        src_ref=src, dst_ref=dst, send_sem=send, recv_sem=recv,
        device_id=target, device_id_type=MESH,
    )


def start_remote(src, dst, send, recv, target):
    copy = remote(src, dst, send, recv, target)
    copy.start()
    return copy


def write_kernel(a, b, c, d, a_out, b_out, c_out, d_out, sems):
    copies = [
        pltpu.make_async_copy(src, dst, sems.at[i])
        for i, (src, dst) in enumerate(((a, a_out), (b, b_out), (c, c_out), (d, d_out)))
    ]
    for copy in copies:
        copy.start()
    for copy in copies:
        copy.wait()


def relay_kernel(
    fwd_hbm, stash_hbm, cot_hbm, win_hbm, wout_hbm, gain_hbm,
    pass_fwd, pass_grad, gin_ref, gout_ref,
    gain_ref, xf, xs, xc, win, wout,
    nf, nb, slope, act_t, dpre_t, act, own_sum, parts, landed,
    mp_out, mp_in, own_terms, z_out,
    load_sem, swap_send, swap_recv, ag_send, ag_recv,
    mp_send, mp_recv, rs_send, rs_recv, z_send, z_recv, above, below, wrapped, entered,
):
    rows = pass_fwd.shape[0]
    tokens = 2 * rows
    hid, width = win.shape
    cols = gin_ref.shape[1]
    n_sec = lax.axis_size("section")
    sec, dp, mp = lax.axis_index("section"), lax.axis_index("dp"), lax.axis_index("mp")
    y, x = lax.div(dp, 2), lax.rem(dp, 2)
    flip_x, flip_y = y * 2 + (1 - x), (1 - y) * 2 + x
    across = (1 - y) * 2 + (1 - x)
    peer = {"mp": 1 - mp}
    after, before = {"section": lax.rem(sec + 1, n_sec)}, {"section": lax.rem(sec + n_sec - 1, n_sec)}
    partner = mp * flip_x + (1 - mp) * flip_y

    barrier = pltpu.get_barrier_semaphore()
    beside = [[{"dp": chip, "mp": core} for core in (mp, 1 - mp)] for chip in (flip_x, flip_y)]

    def signal(sem, target):
        pl.semaphore_signal(sem, inc=1, device_id=target, device_id_type=MESH)

    signal(barrier, peer)
    for low, targets in zip((x == 0, y == 0), beside):
        @pl.when(low)
        def _(targets=targets):
            for target in targets:
                signal(barrier, target)

    @pl.when(sec < n_sec - 1)
    def _():
        signal(barrier, after)

    own, other = pl.ds(0, rows), pl.ds(rows, rows)
    near, far = pl.ds(0, tokens), pl.ds(tokens, tokens)
    local = (
        (stash_hbm, xs.at[own]), (cot_hbm, xc.at[own]), (fwd_hbm, xf.at[own]),
        (gain_hbm, gain_ref), (win_hbm, win), (wout_hbm, wout),
    )
    loads = [
        pltpu.make_async_copy(src, dst, load_sem.at[i]) for i, (src, dst) in enumerate(local)
    ]
    for load in loads:
        load.start()
    load_stash, load_cot, load_fwd, load_gain, load_win, load_wout = loads
    pl.semaphore_wait(barrier, 1 + 2 * x + 2 * y + jnp.minimum(sec, 1))
    for i, (high, targets) in enumerate(zip((x == 1, y == 1), beside)):
        @pl.when(high)
        def _(i=i, targets=targets):
            for target in targets:
                signal(entered.at[i], target)

    load_stash.wait()

    def column(block):
        return pl.ds(pl.multiple_of(block * cols, cols), cols)

    targets = (
        ({"dp": flip_x, "mp": 0}, (across, flip_x, dp, flip_y)),
        ({"dp": flip_y, "mp": 1}, (across, flip_y, dp, flip_x)),
    )
    slot = pl.ds(pl.multiple_of(tokens + mp * rows, rows), rows)
    gathers = []
    for d, (target, _) in enumerate(targets):
        gathers.append(
            remote(xs.at[own], xs.at[slot], ag_send.at[d, 0], ag_recv.at[mp, 0], target)
        )
    for d, copy in enumerate(gathers):
        @pl.when((x, y)[d] == 1)
        def _(copy=copy):
            copy.start()

    for d, copy in enumerate(gathers):
        @pl.when((x, y)[d] == 0)
        def _(d=d, copy=copy):
            pl.semaphore_wait(entered.at[d], 2)
            copy.start()

    load_fwd.wait()
    swap_fwd = start_remote(xf.at[own], xf.at[other], swap_send.at[0], swap_recv.at[0], peer)
    load_cot.wait()
    swap_stash = start_remote(xs.at[own], xs.at[other], swap_send.at[1], swap_recv.at[1], peer)
    swap_cot = start_remote(xc.at[own], xc.at[other], swap_send.at[2], swap_recv.at[2], peer)
    for i in range(4):
        for d, (target, order) in enumerate(targets):
            at = column(order[i])
            gathers.append(
                start_remote(
                    xc.at[own, at], xc.at[slot, at],
                    ag_send.at[d, 1 + i], ag_recv.at[mp, 1 + i], target,
                )
            )

    @pl.when(sec > 0)
    def _():
        signal(above, before)

    @pl.when((sec == 1) & (sec < n_sec - 1))
    def _():
        pl.semaphore_wait(above, 1)
        signal(below, after)

    gathered = (partner, dp, (1 - mp) * flip_x + mp * flip_y, across)

    def await_gather(i):
        for core in range(2):
            rows_at = pl.ds(tokens + core * rows, rows)
            if i == 0:
                src, dst = xs.at[own], xs.at[rows_at]
            else:
                at = column(gathered[i - 1])
                src, dst = xc.at[own, at], xc.at[rows_at, at]
            remote(src, dst, ag_send.at[0, i], ag_recv.at[core, i], peer).wait_recv()

    step = tile_of(rows, 64)

    def normalise(source, target, first, count):
        def body(i, carry):
            at = pl.ds(pl.multiple_of(first + i * step, step), step)
            v = source[at, :].astype(jnp.float32)
            r = lax.rsqrt(jnp.mean(v * v, axis=-1, keepdims=True) + norm_eps)
            target[at, :] = (v * r * gain_ref[...]).astype(jnp.bfloat16)
            return carry

        lax.fori_loop(0, count // step, body, 0)

    block = tile_of(hid, 256)

    def backward_pre(span):
        def body(i, carry):
            at = pl.ds(pl.multiple_of(i * block, block), block)
            v = lax.dot_general(
                win[at, :], nb[span, :], NT, preferred_element_type=jnp.float32
            )
            square = v * v
            t = jnp.tanh(gelu_coef * (v + 0.044715 * square * v))
            act_t[at, span] = (0.5 * v * (1.0 + t)).astype(jnp.bfloat16)
            slope[at, :] = 0.5 * (1.0 + t) + 0.5 * v * (1.0 - t * t) * gelu_coef * (
                1.0 + 0.134145 * square
            )
            return carry

        lax.fori_loop(0, hid // block, body, 0)

    def backward_slope(span, first, count):
        size = tile_of(count, 256)

        def body(i, carry):
            at = pl.ds(pl.multiple_of(first + i * size, size), size)
            d_act = lax.dot_general(
                wout[at, :], xc[span, :], NT, preferred_element_type=jnp.float32
            )
            dpre_t[at, span] = (d_act * slope[at, :]).astype(jnp.bfloat16)
            return carry

        lax.fori_loop(0, count // size, body, 0)

    def forward(span):
        def body(i, carry):
            at = pl.ds(pl.multiple_of(i * block, block), block)
            v = lax.dot_general(
                nf[span, :], win[at, :], NT, preferred_element_type=jnp.float32
            )
            t = jnp.tanh(gelu_coef * (v + 0.044715 * v * v * v))
            act[:, at] = (0.5 * v * (1.0 + t)).astype(jnp.bfloat16)
            return carry

        lax.fori_loop(0, hid // block, body, 0)
        return jnp.dot(
            act[...], wout[...], preferred_element_type=jnp.float32
        ).astype(jnp.bfloat16)

    load_gain.wait()
    normalise(xf, nf, 0, rows)
    load_win.wait()
    load_wout.wait()
    swap_fwd.wait_recv()
    normalise(xf, nf, rows, rows)
    mp_out[1] = forward(other)
    swap_branch = start_remote(mp_out.at[1], mp_in.at[1], mp_send.at[1], mp_recv.at[1], peer)

    @pl.when((sec > 1) & (sec < n_sec - 1))
    def _():
        pl.semaphore_wait(above, 1)
        pl.semaphore_wait(below, 1)
        signal(below, after)

    own_terms[1] = forward(own)
    swap_branch.wait_recv()

    def finish_forward(i, carry):
        at = pl.ds(pl.multiple_of(i * step, step), step)
        branch = own_terms[1, at, :].astype(jnp.float32) + mp_in[1, at, :].astype(jnp.float32)
        z_out[1, at, :] = (xf[at, :].astype(jnp.float32) + branch).astype(jnp.bfloat16)
        return carry

    lax.fori_loop(0, rows // step, finish_forward, 0)

    @pl.when(sec == 0)
    def _():
        pl.semaphore_wait(above, 1)

    if n_sec > 2:
        @pl.when(sec == n_sec - 1)
        def _():
            pl.semaphore_wait(below, 1)

    @pl.when(sec == n_sec - 1)
    def _():
        signal(wrapped, after)

    relay_fwd = start_remote(z_out.at[1], pass_fwd, z_send.at[1], z_recv.at[1], after)

    swap_stash.wait_recv()
    normalise(xs, nb, 0, tokens)
    backward_pre(near)
    swap_cot.wait_recv()
    backward_slope(near, 0, hid)

    def d_norm(span):
        return lax.dot_general(
            dpre_t[:, span], win[...], TN, preferred_element_type=jnp.float32
        ).astype(jnp.bfloat16)

    mp_out[0] = d_norm(other)
    swap_grad = start_remote(mp_out.at[0], mp_in.at[0], mp_send.at[0], mp_recv.at[0], peer)
    own_terms[0] = d_norm(own)
    swap_grad.wait_recv()

    def finish_grad(i, carry):
        at = pl.ds(pl.multiple_of(i * step, step), step)
        v = xs[at, :].astype(jnp.float32)
        r = lax.rsqrt(jnp.mean(v * v, axis=-1, keepdims=True) + norm_eps)
        push = (
            own_terms[0, at, :].astype(jnp.float32) + mp_in[0, at, :].astype(jnp.float32)
        ) * gain_ref[...]
        mixed = jnp.mean(v * push, axis=-1, keepdims=True)
        dx = xc[at, :].astype(jnp.float32) + r * push - v * (r * r * r * mixed)
        z_out[0, at, :] = dx.astype(jnp.bfloat16)
        return carry

    lax.fori_loop(0, rows // step, finish_grad, 0)

    @pl.when(sec == 0)
    def _():
        pl.semaphore_wait(wrapped, 1)

    relay_grad = start_remote(z_out.at[0], pass_grad, z_send.at[0], z_recv.at[0], before)

    operands = {OUT: (act_t, xc), IN: (dpre_t, nb)}
    size = hid // pieces
    bands = [pl.ds(p * size, size) for p in range(pieces)]
    sent = {}

    def product(g, p, owner):
        left, right = operands[g]
        return jnp.dot(
            left[bands[p], :], right[:, column(owner)], preferred_element_type=jnp.float32
        )

    def give(g):
        for p in range(pieces):
            if g == IN:
                backward_slope(far, p * size, size)
            parts[g, bands[p], :] = product(g, p, partner).astype(jnp.bfloat16)
            sent[g, p] = start_remote(
                parts.at[g, bands[p]], landed.at[g, bands[p]],
                rs_send.at[g, p], rs_recv.at[g, p], {"dp": partner},
            )

    def keep(g):
        for p in range(pieces):
            own_sum[g, bands[p], :] = product(g, p, dp)

    await_gather(0)
    normalise(xs, nb, tokens, tokens)
    backward_pre(far)
    await_gather(1)
    give(OUT)
    await_gather(2)
    keep(OUT)
    await_gather(3)
    await_gather(4)
    give(IN)
    keep(IN)

    for g, result in ((OUT, gout_ref), (IN, gin_ref)):
        for p in range(pieces):
            sent[g, p].wait_recv()
            result[bands[p], :] = (
                own_sum[g, bands[p], :] + landed[g, bands[p], :].astype(jnp.float32)
            ).astype(jnp.bfloat16)

    relay_grad.wait_recv()
    relay_fwd.wait_recv()
    for copy in [
        swap_fwd, swap_stash, swap_cot, *gathers, swap_grad, swap_branch,
        relay_grad, relay_fwd, *sent.values(),
    ]:
        copy.wait_send()


def relay_on_device(fwd_in, stash, cot, w_in, w_out, gain):
    rows, width = stash.shape[1:]
    hid = w_in.shape[1]
    tokens = rows * lax.axis_size("mp")
    cols = width // lax.axis_size("dp")
    bf16 = jnp.bfloat16
    vmem = pl.BlockSpec(memory_space=pltpu.VMEM)
    hbm = pl.BlockSpec(memory_space=pl.ANY)
    dma = pltpu.SemaphoreType.DMA
    held = (rows * width + hid * cols) * 2 * jnp.dtype(bf16).itemsize
    results = pl.pallas_call(
        relay_kernel,
        out_shape=(pltpu.VMEM((rows, width), bf16),) * 2 + (pltpu.VMEM((hid, cols), bf16),) * 2,
        in_specs=[hbm] * 6,
        out_specs=(vmem,) * 4,
        scratch_shapes=[
            pltpu.VMEM((1, width), jnp.float32),
            pltpu.VMEM((tokens, width), bf16),
            pltpu.VMEM((2 * tokens, width), bf16),
            pltpu.VMEM((2 * tokens, width), bf16),
            pltpu.VMEM((hid, width), bf16),
            pltpu.VMEM((hid, width), bf16),
            pltpu.VMEM((tokens, width), bf16),
            pltpu.VMEM((2 * tokens, width), bf16),
            pltpu.VMEM((hid, tokens), jnp.float32),
            pltpu.VMEM((hid, 2 * tokens), bf16),
            pltpu.VMEM((hid, 2 * tokens), bf16),
            pltpu.VMEM((rows, hid), bf16),
            pltpu.VMEM((2, hid, cols), jnp.float32),
            pltpu.VMEM((2, hid, cols), bf16),
            pltpu.VMEM((2, hid, cols), bf16),
            pltpu.VMEM((2, rows, width), bf16),
            pltpu.VMEM((2, rows, width), bf16),
            pltpu.VMEM((2, rows, width), bf16),
            pltpu.VMEM((2, rows, width), bf16),
            dma((6,)),
            dma((3,)),
            dma((3,)),
            dma((2, 5)),
            dma((2, 5)),
            dma((2,)),
            dma((2,)),
            dma((2, pieces)),
            dma((2, pieces)),
            dma((2,)),
            dma((2,)),
            *[pltpu.SemaphoreType.REGULAR] * 3,
            pltpu.SemaphoreType.REGULAR((2,)),
        ],
        compiler_params=pltpu.CompilerParams(
            collective_id=0, has_side_effects=True,
            vmem_limit_bytes=vmem_bytes - held - 2**17,
        ),
    )(fwd_in[0], stash[0], cot[0], w_in[0], w_out[0], gain)
    results = pl.pallas_call(
        write_kernel,
        out_shape=tuple(jax.ShapeDtypeStruct(r.shape, r.dtype) for r in results),
        in_specs=[vmem] * 4,
        out_specs=(hbm,) * 4,
        scratch_shapes=[dma((4,))],
        compiler_params=pltpu.CompilerParams(vmem_limit_bytes=4 * 2**20),
    )(*results)
    return tuple(r[None] for r in results)


def fits_relay(mesh):
    return mesh.shape["dp"] == 4 and mesh.shape["mp"] == 2 and mesh.shape["section"] > 1


def solution(mesh):
    in_specs = (
        P("section", ("dp", "mp"), None),
        P("section", ("dp", "mp"), None),
        P("section", ("dp", "mp"), None),
        P("section", "mp", None),
        P("section", "mp", None),
        P("section", None),
    )
    out_specs = (
        P("section", ("dp", "mp"), None),
        P("section", ("dp", "mp"), None),
        P("section", "mp", "dp"),
        P("section", "mp", "dp"),
    )
    return jax.shard_map(
        relay_on_device if fits_relay(mesh) else on_device,
        mesh=mesh,
        in_specs=in_specs,
        out_specs=out_specs,
        check_vma=False,
    )
```

```python
import jax
import jax.numpy as jnp
from jax import lax
from jax.experimental import pallas as pl
from jax.experimental.pallas import tpu as pltpu
from jax.sharding import PartitionSpec as P

norm_eps = 1e-05
gelu_coef = 0.7978845608

def shifted(x, axis, by):
    length = lax.axis_size(axis)
    return lax.ppermute(x, axis, [(i, (i + by) % length) for i in range(length)])

def gelu_value(v):
    inner = jnp.tanh(gelu_coef * (v + 0.044715 * v * v * v))
    return 0.5 * v * (1.0 + inner)

def gelu_slope(v):
    inner = jnp.tanh(gelu_coef * (v + 0.044715 * v * v * v))
    return 0.5 * (1.0 + inner) + 0.5 * v * (1.0 - inner * inner) * gelu_coef * (
        1.0 + 0.134145 * v * v
    )

def prepare(x, w_first, gain_row):
    xf = x.astype(jnp.float32)
    scale = lax.rsqrt(jnp.mean(xf * xf, axis=-1, keepdims=True) + norm_eps)
    normed = (xf * scale * gain_row[None, :]).astype(jnp.bfloat16)
    pre = lax.dot_general(
        normed, w_first, (((1,), (1,)), ((), ())), preferred_element_type=jnp.float32
    )
    act = gelu_value(pre).astype(jnp.bfloat16)
    return (scale, normed, pre, act)

def on_device(fwd_in, stash, cot, w_in, w_out, gain):
    x_fwd = fwd_in[0]
    x_bwd = stash[0]
    cot_local = cot[0]
    w_first = w_in[0]
    w_second = w_out[0]
    gain_row = gain[0]
    local_rows = x_fwd.shape[0]
    scale, normed, pre, act = prepare(
        lax.all_gather(x_fwd, "mp", axis=0, tiled=True), w_first, gain_row
    )
    terms = jnp.dot(act, w_second, preferred_element_type=jnp.float32)
    branch = lax.psum_scatter(
        terms.astype(jnp.bfloat16), "mp", scatter_dimension=0, tiled=True
    ).astype(jnp.float32)
    out = (x_fwd.astype(jnp.float32) + branch).astype(jnp.bfloat16)
    passed_fwd = shifted(out, "section", 1)
    rows_x, rows_cot = (
        lax.all_gather(x_bwd, "mp", axis=0, tiled=True),
        lax.all_gather(cot_local, "mp", axis=0, tiled=True),
    )
    scale, normed, pre, act = prepare(rows_x, w_first, gain_row)
    d_act = lax.dot_general(
        rows_cot, w_second, (((1,), (1,)), ((), ())), preferred_element_type=jnp.float32
    )
    d_pre = (d_act * gelu_slope(pre)).astype(jnp.bfloat16)
    d_norm = lax.psum_scatter(
        jnp.dot(d_pre, w_first, preferred_element_type=jnp.float32).astype(jnp.bfloat16),
        "mp",
        scatter_dimension=0,
        tiled=True,
    ).astype(jnp.float32)
    offset = lax.axis_index("mp") * local_rows
    own_scale = lax.dynamic_slice_in_dim(scale, offset, local_rows, 0)
    shard_x = x_bwd.astype(jnp.float32)
    push = d_norm * gain_row[None, :]
    mixed = jnp.mean(shard_x * push, axis=-1, keepdims=True)
    dx = (
        cot_local.astype(jnp.float32)
        + own_scale * push
        - shard_x * own_scale * own_scale * own_scale * mixed
    )
    passed_grad = shifted(dx.astype(jnp.bfloat16), "section", -1)
    term_out = lax.dot_general(
        act, rows_cot, (((0,), (0,)), ((), ())), preferred_element_type=jnp.float32
    )
    term_in = lax.dot_general(
        d_pre, normed, (((0,), (0,)), ((), ())), preferred_element_type=jnp.float32
    )
    sum_in, sum_out = (
        lax.psum_scatter(
            term_in.astype(jnp.bfloat16), "dp", scatter_dimension=1, tiled=True
        ).astype(jnp.float32),
        lax.psum_scatter(
            term_out.astype(jnp.bfloat16), "dp", scatter_dimension=1, tiled=True
        ).astype(jnp.float32),
    )
    return (
        passed_fwd[None],
        passed_grad[None],
        sum_in.astype(jnp.bfloat16)[None],
        sum_out.astype(jnp.bfloat16)[None],
    )

MESH = pl.DeviceIdType.MESH
vmem_bytes = 67_043_328
NT = (((1,), (1,)), ((), ()))
TN = (((0,), (0,)), ((), ()))
OUT, IN = range(2)
pieces = 4

def tile_of(total, most):
    size = min(total, most)
    while total % size:
        size //= 2
    return size

def remote(src, dst, send, recv, target):
    return pltpu.make_async_remote_copy(
        src_ref=src, dst_ref=dst, send_sem=send, recv_sem=recv,
        device_id=target, device_id_type=MESH,
    )

def start_remote(src, dst, send, recv, target):
    copy = remote(src, dst, send, recv, target)
    copy.start()
    return copy

def write_kernel(a, b, c, d, a_out, b_out, c_out, d_out, sems):
    copies = [
        pltpu.make_async_copy(src, dst, sems.at[i])
        for i, (src, dst) in enumerate(((a, a_out), (b, b_out), (c, c_out), (d, d_out)))
    ]
    for copy in copies:
        copy.start()
    for copy in copies:
        copy.wait()

def relay_kernel(
    fwd_hbm, stash_hbm, cot_hbm, win_hbm, wout_hbm, gain_hbm,
    pass_fwd, pass_grad, gin_ref, gout_ref,
    gain_ref, xf, xs, xc, win, wout,
    nf, nb, slope, act_t, dpre_t, act, own_sum, parts, landed,
    mp_out, mp_in, own_terms, z_out,
    load_sem, swap_send, swap_recv, ag_send, ag_recv,
    mp_send, mp_recv, rs_send, rs_recv, z_send, z_recv, above, below, wrapped, entered,
):
    rows = pass_fwd.shape[0]
    tokens = 2 * rows
    hid, width = win.shape
    cols = gin_ref.shape[1]
    n_sec = lax.axis_size("section")
    sec, dp, mp = lax.axis_index("section"), lax.axis_index("dp"), lax.axis_index("mp")
    y, x = lax.div(dp, 2), lax.rem(dp, 2)
    flip_x, flip_y = y * 2 + (1 - x), (1 - y) * 2 + x
    across = (1 - y) * 2 + (1 - x)
    peer = {"mp": 1 - mp}
    after, before = {"section": lax.rem(sec + 1, n_sec)}, {"section": lax.rem(sec + n_sec - 1, n_sec)}
    partner = mp * flip_x + (1 - mp) * flip_y

    barrier = pltpu.get_barrier_semaphore()
    beside = [[{"dp": chip, "mp": core} for core in (mp, 1 - mp)] for chip in (flip_x, flip_y)]

    def signal(sem, target):
        pl.semaphore_signal(sem, inc=1, device_id=target, device_id_type=MESH)

    @pl.when(mp == 1)
    def _():
        signal(barrier, peer)

    for low, targets in zip((x == 0, y == 0), beside):
        @pl.when(low)
        def _(targets=targets):
            for target in targets:
                signal(barrier, target)

    @pl.when(sec < n_sec - 1)
    def _():
        signal(barrier, after)

    own, other = pl.ds(0, rows), pl.ds(rows, rows)
    near, far = pl.ds(0, tokens), pl.ds(tokens, tokens)
    local = (
        (stash_hbm, xs.at[own]), (cot_hbm, xc.at[own]), (fwd_hbm, xf.at[own]),
        (gain_hbm, gain_ref), (win_hbm, win), (wout_hbm, wout),
    )
    loads = [
        pltpu.make_async_copy(src, dst, load_sem.at[i]) for i, (src, dst) in enumerate(local)
    ]
    for load in loads:
        load.start()
    load_stash, load_cot, load_fwd, load_gain, load_win, load_wout = loads
    awaited = 1 - mp + 2 * x + 2 * y + jnp.minimum(sec, 1)

    @pl.when(awaited > 0)
    def _():
        pl.semaphore_wait(barrier, awaited)

    @pl.when(mp == 0)
    def _():
        signal(entered.at[2], peer)

    for i, (high, targets) in enumerate(zip((x == 1, y == 1), beside)):
        @pl.when(high)
        def _(i=i, targets=targets):
            for target in targets:
                signal(entered.at[i], target)

    def column(block):
        return pl.ds(pl.multiple_of(block * cols, cols), cols)

    targets = (
        ({"dp": flip_x, "mp": 0}, (across, flip_x, dp, flip_y)),
        ({"dp": flip_y, "mp": 1}, (across, flip_y, dp, flip_x)),
    )
    slot = pl.ds(pl.multiple_of(tokens + mp * rows, rows), rows)
    gathers = []
    for d, (target, _) in enumerate(targets):
        gathers.append(
            remote(stash_hbm, xs.at[slot], ag_send.at[d, 0], ag_recv.at[mp, 0], target)
        )
    for d, copy in enumerate(gathers):
        @pl.when((x, y)[d] == 1)
        def _(copy=copy):
            copy.start()

    for d, copy in enumerate(gathers):
        @pl.when((x, y)[d] == 0)
        def _(d=d, copy=copy):
            pl.semaphore_wait(entered.at[d], 2)
            copy.start()

    @pl.when(mp == 1)
    def _():
        pl.semaphore_wait(entered.at[2], 1)

    load_fwd.wait()
    swap_fwd = start_remote(xf.at[own], xf.at[other], swap_send.at[0], swap_recv.at[0], peer)
    load_stash.wait()
    load_cot.wait()
    swap_stash = start_remote(xs.at[own], xs.at[other], swap_send.at[1], swap_recv.at[1], peer)
    swap_cot = start_remote(xc.at[own], xc.at[other], swap_send.at[2], swap_recv.at[2], peer)
    for i in range(4):
        for d, (target, order) in enumerate(targets):
            at = column(order[i])
            gathers.append(
                start_remote(
                    xc.at[own, at], xc.at[slot, at],
                    ag_send.at[d, 1 + i], ag_recv.at[mp, 1 + i], target,
                )
            )

    @pl.when(sec > 0)
    def _():
        signal(above, before)

    @pl.when((sec == 1) & (sec < n_sec - 1))
    def _():
        pl.semaphore_wait(above, 1)
        signal(below, after)

    gathered = (partner, dp, (1 - mp) * flip_x + mp * flip_y, across)

    def await_gather(i):
        for core in range(2):
            rows_at = pl.ds(tokens + core * rows, rows)
            if i == 0:
                src, dst = xs.at[own], xs.at[rows_at]
            else:
                at = column(gathered[i - 1])
                src, dst = xc.at[own, at], xc.at[rows_at, at]
            remote(src, dst, ag_send.at[0, i], ag_recv.at[core, i], peer).wait_recv()

    step = tile_of(rows, 64)

    def normalise(source, target, first, count):
        def body(i, carry):
            at = pl.ds(pl.multiple_of(first + i * step, step), step)
            v = source[at, :].astype(jnp.float32)
            r = lax.rsqrt(jnp.mean(v * v, axis=-1, keepdims=True) + norm_eps)
            target[at, :] = (v * r * gain_ref[...]).astype(jnp.bfloat16)
            return carry

        lax.fori_loop(0, count // step, body, 0)

    block = tile_of(hid, 256)

    def backward_pre(span):
        def body(i, carry):
            at = pl.ds(pl.multiple_of(i * block, block), block)
            v = lax.dot_general(
                win[at, :], nb[span, :], NT, preferred_element_type=jnp.float32
            )
            square = v * v
            t = jnp.tanh(gelu_coef * (v + 0.044715 * square * v))
            act_t[at, span] = (0.5 * v * (1.0 + t)).astype(jnp.bfloat16)
            slope[at, :] = 0.5 * (1.0 + t) + 0.5 * v * (1.0 - t * t) * gelu_coef * (
                1.0 + 0.134145 * square
            )
            return carry

        lax.fori_loop(0, hid // block, body, 0)

    def backward_slope(span, first, count):
        size = tile_of(count, 256)

        def body(i, carry):
            at = pl.ds(pl.multiple_of(first + i * size, size), size)
            d_act = lax.dot_general(
                wout[at, :], xc[span, :], NT, preferred_element_type=jnp.float32
            )
            dpre_t[at, span] = (d_act * slope[at, :]).astype(jnp.bfloat16)
            return carry

        lax.fori_loop(0, count // size, body, 0)

    def forward(span):
        def body(i, carry):
            at = pl.ds(pl.multiple_of(i * block, block), block)
            v = lax.dot_general(
                nf[span, :], win[at, :], NT, preferred_element_type=jnp.float32
            )
            t = jnp.tanh(gelu_coef * (v + 0.044715 * v * v * v))
            act[:, at] = (0.5 * v * (1.0 + t)).astype(jnp.bfloat16)
            return carry

        lax.fori_loop(0, hid // block, body, 0)
        return jnp.dot(
            act[...], wout[...], preferred_element_type=jnp.float32
        ).astype(jnp.bfloat16)

    load_gain.wait()
    normalise(xf, nf, 0, rows)
    load_win.wait()
    load_wout.wait()
    swap_fwd.wait_recv()
    normalise(xf, nf, rows, rows)
    mp_out[1] = forward(other)
    swap_branch = start_remote(mp_out.at[1], mp_in.at[1], mp_send.at[1], mp_recv.at[1], peer)

    @pl.when((sec > 1) & (sec < n_sec - 1))
    def _():
        pl.semaphore_wait(above, 1)
        pl.semaphore_wait(below, 1)
        signal(below, after)

    own_terms[1] = forward(own)
    swap_branch.wait_recv()

    def finish_forward(i, carry):
        at = pl.ds(pl.multiple_of(i * step, step), step)
        branch = own_terms[1, at, :].astype(jnp.float32) + mp_in[1, at, :].astype(jnp.float32)
        z_out[1, at, :] = (xf[at, :].astype(jnp.float32) + branch).astype(jnp.bfloat16)
        return carry

    lax.fori_loop(0, rows // step, finish_forward, 0)

    @pl.when(sec == 0)
    def _():
        pl.semaphore_wait(above, 1)

    if n_sec > 2:
        @pl.when(sec == n_sec - 1)
        def _():
            pl.semaphore_wait(below, 1)

    @pl.when(sec == n_sec - 1)
    def _():
        signal(wrapped, after)

    relay_fwd = start_remote(z_out.at[1], pass_fwd, z_send.at[1], z_recv.at[1], after)

    swap_stash.wait_recv()
    normalise(xs, nb, 0, tokens)
    backward_pre(near)
    swap_cot.wait_recv()
    backward_slope(near, 0, hid)

    def d_norm(span):
        return lax.dot_general(
            dpre_t[:, span], win[...], TN, preferred_element_type=jnp.float32
        ).astype(jnp.bfloat16)

    mp_out[0] = d_norm(other)
    swap_grad = start_remote(mp_out.at[0], mp_in.at[0], mp_send.at[0], mp_recv.at[0], peer)
    own_terms[0] = d_norm(own)
    swap_grad.wait_recv()

    def finish_grad(i, carry):
        at = pl.ds(pl.multiple_of(i * step, step), step)
        v = xs[at, :].astype(jnp.float32)
        r = lax.rsqrt(jnp.mean(v * v, axis=-1, keepdims=True) + norm_eps)
        push = (
            own_terms[0, at, :].astype(jnp.float32) + mp_in[0, at, :].astype(jnp.float32)
        ) * gain_ref[...]
        mixed = jnp.mean(v * push, axis=-1, keepdims=True)
        dx = xc[at, :].astype(jnp.float32) + r * push - v * (r * r * r * mixed)
        z_out[0, at, :] = dx.astype(jnp.bfloat16)
        return carry

    lax.fori_loop(0, rows // step, finish_grad, 0)

    @pl.when(sec == 0)
    def _():
        pl.semaphore_wait(wrapped, 1)

    relay_grad = start_remote(z_out.at[0], pass_grad, z_send.at[0], z_recv.at[0], before)

    operands = {OUT: (act_t, xc), IN: (dpre_t, nb)}
    size = hid // pieces
    bands = [pl.ds(p * size, size) for p in range(pieces)]
    sent = {}

    def product(g, p, owner):
        left, right = operands[g]
        return jnp.dot(
            left[bands[p], :], right[:, column(owner)], preferred_element_type=jnp.float32
        )

    def give(g):
        for p in range(pieces):
            if g == IN:
                backward_slope(far, p * size, size)
            parts[g, bands[p], :] = product(g, p, partner).astype(jnp.bfloat16)
            sent[g, p] = start_remote(
                parts.at[g, bands[p]], landed.at[g, bands[p]],
                rs_send.at[g, p], rs_recv.at[g, p], {"dp": partner},
            )

    def keep(g):
        for p in range(pieces):
            own_sum[g, bands[p], :] = product(g, p, dp)

    await_gather(0)
    normalise(xs, nb, tokens, tokens)
    backward_pre(far)
    await_gather(1)
    give(OUT)
    await_gather(2)
    keep(OUT)
    await_gather(3)
    await_gather(4)
    give(IN)
    keep(IN)

    for copy in [swap_fwd, swap_stash, swap_cot, *gathers, swap_grad, swap_branch]:
        copy.wait_send()
    for g, result in ((OUT, gout_ref), (IN, gin_ref)):
        for p in range(pieces):
            if (g, p) == (IN, pieces - 1):
                for copy in (relay_grad, relay_fwd):
                    copy.wait()
            sent[g, p].wait()
            result[bands[p], :] = (
                own_sum[g, bands[p], :] + landed[g, bands[p], :].astype(jnp.float32)
            ).astype(jnp.bfloat16)

def relay_on_device(fwd_in, stash, cot, w_in, w_out, gain):
    rows, width = stash.shape[1:]
    hid = w_in.shape[1]
    tokens = rows * lax.axis_size("mp")
    cols = width // lax.axis_size("dp")
    bf16 = jnp.bfloat16
    vmem = pl.BlockSpec(memory_space=pltpu.VMEM)
    hbm = pl.BlockSpec(memory_space=pl.ANY)
    dma = pltpu.SemaphoreType.DMA
    held = (rows * width + hid * cols) * 2 * jnp.dtype(bf16).itemsize
    results = pl.pallas_call(
        relay_kernel,
        out_shape=(pltpu.VMEM((rows, width), bf16),) * 2 + (pltpu.VMEM((hid, cols), bf16),) * 2,
        in_specs=[hbm] * 6,
        out_specs=(vmem,) * 4,
        scratch_shapes=[
            pltpu.VMEM((1, width), jnp.float32),
            pltpu.VMEM((tokens, width), bf16),
            pltpu.VMEM((2 * tokens, width), bf16),
            pltpu.VMEM((2 * tokens, width), bf16),
            pltpu.VMEM((hid, width), bf16),
            pltpu.VMEM((hid, width), bf16),
            pltpu.VMEM((tokens, width), bf16),
            pltpu.VMEM((2 * tokens, width), bf16),
            pltpu.VMEM((hid, tokens), jnp.float32),
            pltpu.VMEM((hid, 2 * tokens), bf16),
            pltpu.VMEM((hid, 2 * tokens), bf16),
            pltpu.VMEM((rows, hid), bf16),
            pltpu.VMEM((2, hid, cols), jnp.float32),
            pltpu.VMEM((2, hid, cols), bf16),
            pltpu.VMEM((2, hid, cols), bf16),
            pltpu.VMEM((2, rows, width), bf16),
            pltpu.VMEM((2, rows, width), bf16),
            pltpu.VMEM((2, rows, width), bf16),
            pltpu.VMEM((2, rows, width), bf16),
            dma((6,)),
            dma((3,)),
            dma((3,)),
            dma((2, 5)),
            dma((2, 5)),
            dma((2,)),
            dma((2,)),
            dma((2, pieces)),
            dma((2, pieces)),
            dma((2,)),
            dma((2,)),
            *[pltpu.SemaphoreType.REGULAR] * 3,
            pltpu.SemaphoreType.REGULAR((3,)),
        ],
        compiler_params=pltpu.CompilerParams(
            collective_id=0, has_side_effects=True,
            vmem_limit_bytes=vmem_bytes - held - 2**17,
        ),
    )(fwd_in[0], stash[0], cot[0], w_in[0], w_out[0], gain)
    results = pl.pallas_call(
        write_kernel,
        out_shape=tuple(jax.ShapeDtypeStruct(r.shape, r.dtype) for r in results),
        in_specs=[vmem] * 4,
        out_specs=(hbm,) * 4,
        scratch_shapes=[dma((4,))],
        compiler_params=pltpu.CompilerParams(vmem_limit_bytes=4 * 2**20),
    )(*results)
    return tuple(r[None] for r in results)

def fits_relay(mesh):
    return mesh.shape["dp"] == 4 and mesh.shape["mp"] == 2 and mesh.shape["section"] > 1

def solution(mesh):
    in_specs = (
        P("section", ("dp", "mp"), None),
        P("section", ("dp", "mp"), None),
        P("section", ("dp", "mp"), None),
        P("section", "mp", None),
        P("section", "mp", None),
        P("section", None),
    )
    out_specs = (
        P("section", ("dp", "mp"), None),
        P("section", ("dp", "mp"), None),
        P("section", "mp", "dp"),
        P("section", "mp", "dp"),
    )
    return jax.shard_map(
        relay_on_device if fits_relay(mesh) else on_device,
        mesh=mesh,
        in_specs=in_specs,
        out_specs=out_specs,
        check_vma=False,
    )
```

```python
import jax
import jax.numpy as jnp
from jax import lax
from jax.experimental import pallas as pl
from jax.experimental.pallas import tpu as pltpu
from jax.sharding import PartitionSpec as P

norm_eps = 1e-05
gelu_coef = 0.7978845608

def shifted(x, axis, by):
    length = lax.axis_size(axis)
    return lax.ppermute(x, axis, [(i, (i + by) % length) for i in range(length)])

def gelu_value(v):
    inner = jnp.tanh(gelu_coef * (v + 0.044715 * v * v * v))
    return 0.5 * v * (1.0 + inner)

def gelu_slope(v):
    inner = jnp.tanh(gelu_coef * (v + 0.044715 * v * v * v))
    return 0.5 * (1.0 + inner) + 0.5 * v * (1.0 - inner * inner) * gelu_coef * (
        1.0 + 0.134145 * v * v
    )

def prepare(x, w_first, gain_row):
    xf = x.astype(jnp.float32)
    scale = lax.rsqrt(jnp.mean(xf * xf, axis=-1, keepdims=True) + norm_eps)
    normed = (xf * scale * gain_row[None, :]).astype(jnp.bfloat16)
    pre = lax.dot_general(
        normed, w_first, (((1,), (1,)), ((), ())), preferred_element_type=jnp.float32
    )
    act = gelu_value(pre).astype(jnp.bfloat16)
    return (scale, normed, pre, act)

def on_device(fwd_in, stash, cot, w_in, w_out, gain):
    x_fwd = fwd_in[0]
    x_bwd = stash[0]
    cot_local = cot[0]
    w_first = w_in[0]
    w_second = w_out[0]
    gain_row = gain[0]
    local_rows = x_fwd.shape[0]
    scale, normed, pre, act = prepare(
        lax.all_gather(x_fwd, "mp", axis=0, tiled=True), w_first, gain_row
    )
    terms = jnp.dot(act, w_second, preferred_element_type=jnp.float32)
    branch = lax.psum_scatter(
        terms.astype(jnp.bfloat16), "mp", scatter_dimension=0, tiled=True
    ).astype(jnp.float32)
    out = (x_fwd.astype(jnp.float32) + branch).astype(jnp.bfloat16)
    passed_fwd = shifted(out, "section", 1)
    rows_x, rows_cot = (
        lax.all_gather(x_bwd, "mp", axis=0, tiled=True),
        lax.all_gather(cot_local, "mp", axis=0, tiled=True),
    )
    scale, normed, pre, act = prepare(rows_x, w_first, gain_row)
    d_act = lax.dot_general(
        rows_cot, w_second, (((1,), (1,)), ((), ())), preferred_element_type=jnp.float32
    )
    d_pre = (d_act * gelu_slope(pre)).astype(jnp.bfloat16)
    d_norm = lax.psum_scatter(
        jnp.dot(d_pre, w_first, preferred_element_type=jnp.float32).astype(jnp.bfloat16),
        "mp",
        scatter_dimension=0,
        tiled=True,
    ).astype(jnp.float32)
    offset = lax.axis_index("mp") * local_rows
    own_scale = lax.dynamic_slice_in_dim(scale, offset, local_rows, 0)
    shard_x = x_bwd.astype(jnp.float32)
    push = d_norm * gain_row[None, :]
    mixed = jnp.mean(shard_x * push, axis=-1, keepdims=True)
    dx = (
        cot_local.astype(jnp.float32)
        + own_scale * push
        - shard_x * own_scale * own_scale * own_scale * mixed
    )
    passed_grad = shifted(dx.astype(jnp.bfloat16), "section", -1)
    term_out = lax.dot_general(
        act, rows_cot, (((0,), (0,)), ((), ())), preferred_element_type=jnp.float32
    )
    term_in = lax.dot_general(
        d_pre, normed, (((0,), (0,)), ((), ())), preferred_element_type=jnp.float32
    )
    sum_in, sum_out = (
        lax.psum_scatter(
            term_in.astype(jnp.bfloat16), "dp", scatter_dimension=1, tiled=True
        ).astype(jnp.float32),
        lax.psum_scatter(
            term_out.astype(jnp.bfloat16), "dp", scatter_dimension=1, tiled=True
        ).astype(jnp.float32),
    )
    return (
        passed_fwd[None],
        passed_grad[None],
        sum_in.astype(jnp.bfloat16)[None],
        sum_out.astype(jnp.bfloat16)[None],
    )

MESH = pl.DeviceIdType.MESH
vmem_bytes = 67_043_328
NT = (((1,), (1,)), ((), ()))
TN = (((0,), (0,)), ((), ()))
OUT, IN = range(2)
pieces = 4

def tile_of(total, most):
    size = min(total, most)
    while total % size:
        size //= 2
    return size

def remote(src, dst, send, recv, target):
    return pltpu.make_async_remote_copy(
        src_ref=src, dst_ref=dst, send_sem=send, recv_sem=recv,
        device_id=target, device_id_type=MESH,
    )

def start_remote(src, dst, send, recv, target):
    copy = remote(src, dst, send, recv, target)
    copy.start()
    return copy

def write_kernel(a, b, c, d, a_out, b_out, c_out, d_out, sems):
    copies = [
        pltpu.make_async_copy(src, dst, sems.at[i])
        for i, (src, dst) in enumerate(((a, a_out), (b, b_out), (c, c_out), (d, d_out)))
    ]
    for copy in copies:
        copy.start()
    for copy in copies:
        copy.wait()

def relay_kernel(
    fwd_hbm, stash_hbm, cot_hbm, win_hbm, wout_hbm, gain_hbm,
    pass_fwd, pass_grad, gin_ref, gout_ref,
    gain_ref, xf, xs, xc, win, wout,
    nf, nb, slope, act_t, dpre_t, act, own_sum, parts, landed,
    mp_out, mp_in, own_terms, z_out,
    load_sem, swap_send, swap_recv, ag_send, ag_recv,
    mp_send, mp_recv, rs_send, rs_recv, z_send, z_recv, above, below, wrapped, entered,
):
    rows = pass_fwd.shape[0]
    tokens = 2 * rows
    hid, width = win.shape
    cols = gin_ref.shape[1]
    n_sec = lax.axis_size("section")
    sec, dp, mp = lax.axis_index("section"), lax.axis_index("dp"), lax.axis_index("mp")
    y, x = lax.div(dp, 2), lax.rem(dp, 2)
    flip_x, flip_y = y * 2 + (1 - x), (1 - y) * 2 + x
    across = (1 - y) * 2 + (1 - x)
    peer = {"mp": 1 - mp}
    after, before = {"section": lax.rem(sec + 1, n_sec)}, {"section": lax.rem(sec + n_sec - 1, n_sec)}
    partner = mp * flip_x + (1 - mp) * flip_y

    barrier = pltpu.get_barrier_semaphore()
    beside = [[{"dp": chip, "mp": core} for core in (mp, 1 - mp)] for chip in (flip_x, flip_y)]

    def signal(sem, target):
        pl.semaphore_signal(sem, inc=1, device_id=target, device_id_type=MESH)

    @pl.when(mp == 1)
    def _():
        signal(barrier, peer)

    for low, targets in zip((x == 0, y == 0), beside):
        @pl.when(low)
        def _(targets=targets):
            for target in targets:
                signal(barrier, target)

    @pl.when(sec < n_sec - 1)
    def _():
        signal(barrier, after)

    own, other = pl.ds(0, rows), pl.ds(rows, rows)
    near, far = pl.ds(0, tokens), pl.ds(tokens, tokens)
    local = (
        (stash_hbm, xs.at[own]), (cot_hbm, xc.at[own]), (fwd_hbm, xf.at[own]),
        (gain_hbm, gain_ref), (win_hbm, win), (wout_hbm, wout),
    )
    loads = [
        pltpu.make_async_copy(src, dst, load_sem.at[i]) for i, (src, dst) in enumerate(local)
    ]
    load_stash, load_cot, load_fwd, load_gain, load_win, load_wout = loads
    awaited = 1 - mp + 2 * x + 2 * y + jnp.minimum(sec, 1)

    @pl.when(awaited > 0)
    def _():
        pl.semaphore_wait(barrier, awaited)

    def column(block):
        return pl.ds(pl.multiple_of(block * cols, cols), cols)

    targets = (
        ({"dp": flip_x, "mp": 0}, (across, flip_x, dp, flip_y)),
        ({"dp": flip_y, "mp": 1}, (across, flip_y, dp, flip_x)),
    )
    slot = pl.ds(pl.multiple_of(tokens + mp * rows, rows), rows)
    gathers = []
    for d, (target, _) in enumerate(targets):
        gathers.append(
            remote(stash_hbm, xs.at[slot], ag_send.at[d, 0], ag_recv.at[mp, 0], target)
        )
    for d, copy in enumerate(gathers):
        @pl.when((x, y)[d] == 1)
        def _(copy=copy):
            copy.start()

    @pl.when(mp == 0)
    def _():
        signal(entered.at[2], peer)

    for i, (high, cores) in enumerate(zip((x == 1, y == 1), beside)):
        @pl.when(high)
        def _(i=i, cores=cores):
            for target in cores:
                signal(entered.at[i], target)

    for load in loads:
        load.start()

    for d, copy in enumerate(gathers):
        @pl.when((x, y)[d] == 0)
        def _(d=d, copy=copy):
            pl.semaphore_wait(entered.at[d], 2)
            copy.start()

    for i in range(4):
        for d, (target, order) in enumerate(targets):
            at = column(order[i])
            gathers.append(
                start_remote(
                    cot_hbm.at[:, at], xc.at[slot, at],
                    ag_send.at[d, 1 + i], ag_recv.at[mp, 1 + i], target,
                )
            )

    @pl.when(mp == 1)
    def _():
        pl.semaphore_wait(entered.at[2], 1)

    load_fwd.wait()
    swap_fwd = start_remote(xf.at[own], xf.at[other], swap_send.at[0], swap_recv.at[0], peer)
    load_stash.wait()
    load_cot.wait()
    swap_stash = start_remote(xs.at[own], xs.at[other], swap_send.at[1], swap_recv.at[1], peer)
    swap_cot = start_remote(xc.at[own], xc.at[other], swap_send.at[2], swap_recv.at[2], peer)
    @pl.when(sec > 0)
    def _():
        signal(above, before)

    @pl.when((sec == 1) & (sec < n_sec - 1))
    def _():
        pl.semaphore_wait(above, 1)
        signal(below, after)

    gathered = (partner, dp, (1 - mp) * flip_x + mp * flip_y, across)

    def await_gather(i):
        for core in range(2):
            rows_at = pl.ds(tokens + core * rows, rows)
            if i == 0:
                src, dst = xs.at[own], xs.at[rows_at]
            else:
                at = column(gathered[i - 1])
                src, dst = xc.at[own, at], xc.at[rows_at, at]
            remote(src, dst, ag_send.at[0, i], ag_recv.at[core, i], peer).wait_recv()

    step = tile_of(rows, 64)

    def normalise(source, target, first, count):
        def body(i, carry):
            at = pl.ds(pl.multiple_of(first + i * step, step), step)
            v = source[at, :].astype(jnp.float32)
            r = lax.rsqrt(jnp.mean(v * v, axis=-1, keepdims=True) + norm_eps)
            target[at, :] = (v * r * gain_ref[...]).astype(jnp.bfloat16)
            return carry

        lax.fori_loop(0, count // step, body, 0)

    block = tile_of(hid, 256)

    def backward_pre(span):
        def body(i, carry):
            at = pl.ds(pl.multiple_of(i * block, block), block)
            v = lax.dot_general(
                win[at, :], nb[span, :], NT, preferred_element_type=jnp.float32
            )
            square = v * v
            t = jnp.tanh(gelu_coef * (v + 0.044715 * square * v))
            act_t[at, span] = (0.5 * v * (1.0 + t)).astype(jnp.bfloat16)
            slope[at, :] = 0.5 * (1.0 + t) + 0.5 * v * (1.0 - t * t) * gelu_coef * (
                1.0 + 0.134145 * square
            )
            return carry

        lax.fori_loop(0, hid // block, body, 0)

    def backward_slope(span, first, count):
        size = tile_of(count, 256)

        def body(i, carry):
            at = pl.ds(pl.multiple_of(first + i * size, size), size)
            d_act = lax.dot_general(
                wout[at, :], xc[span, :], NT, preferred_element_type=jnp.float32
            )
            dpre_t[at, span] = (d_act * slope[at, :]).astype(jnp.bfloat16)
            return carry

        lax.fori_loop(0, count // size, body, 0)

    def forward(span):
        def body(i, carry):
            at = pl.ds(pl.multiple_of(i * block, block), block)
            v = lax.dot_general(
                nf[span, :], win[at, :], NT, preferred_element_type=jnp.float32
            )
            t = jnp.tanh(gelu_coef * (v + 0.044715 * v * v * v))
            act[:, at] = (0.5 * v * (1.0 + t)).astype(jnp.bfloat16)
            return carry

        lax.fori_loop(0, hid // block, body, 0)
        return jnp.dot(
            act[...], wout[...], preferred_element_type=jnp.float32
        ).astype(jnp.bfloat16)

    load_gain.wait()
    normalise(xf, nf, 0, rows)
    load_win.wait()
    load_wout.wait()
    swap_fwd.wait_recv()
    normalise(xf, nf, rows, rows)
    mp_out[1] = forward(other)
    swap_branch = start_remote(mp_out.at[1], mp_in.at[1], mp_send.at[1], mp_recv.at[1], peer)

    @pl.when((sec > 1) & (sec < n_sec - 1))
    def _():
        pl.semaphore_wait(above, 1)
        pl.semaphore_wait(below, 1)
        signal(below, after)

    own_terms[1] = forward(own)
    swap_branch.wait_recv()

    def finish_forward(i, carry):
        at = pl.ds(pl.multiple_of(i * step, step), step)
        branch = own_terms[1, at, :].astype(jnp.float32) + mp_in[1, at, :].astype(jnp.float32)
        z_out[1, at, :] = (xf[at, :].astype(jnp.float32) + branch).astype(jnp.bfloat16)
        return carry

    lax.fori_loop(0, rows // step, finish_forward, 0)

    @pl.when(sec == 0)
    def _():
        pl.semaphore_wait(above, 1)

    if n_sec > 2:
        @pl.when(sec == n_sec - 1)
        def _():
            pl.semaphore_wait(below, 1)

    @pl.when(sec == n_sec - 1)
    def _():
        signal(wrapped, after)

    relay_fwd = start_remote(z_out.at[1], pass_fwd, z_send.at[1], z_recv.at[1], after)

    swap_stash.wait_recv()
    normalise(xs, nb, 0, tokens)
    backward_pre(near)
    swap_cot.wait_recv()
    backward_slope(near, 0, hid)

    def d_norm(span):
        return lax.dot_general(
            dpre_t[:, span], win[...], TN, preferred_element_type=jnp.float32
        ).astype(jnp.bfloat16)

    mp_out[0] = d_norm(other)
    swap_grad = start_remote(mp_out.at[0], mp_in.at[0], mp_send.at[0], mp_recv.at[0], peer)
    own_terms[0] = d_norm(own)
    swap_grad.wait_recv()

    def finish_grad(i, carry):
        at = pl.ds(pl.multiple_of(i * step, step), step)
        v = xs[at, :].astype(jnp.float32)
        r = lax.rsqrt(jnp.mean(v * v, axis=-1, keepdims=True) + norm_eps)
        push = (
            own_terms[0, at, :].astype(jnp.float32) + mp_in[0, at, :].astype(jnp.float32)
        ) * gain_ref[...]
        mixed = jnp.mean(v * push, axis=-1, keepdims=True)
        dx = xc[at, :].astype(jnp.float32) + r * push - v * (r * r * r * mixed)
        z_out[0, at, :] = dx.astype(jnp.bfloat16)
        return carry

    lax.fori_loop(0, rows // step, finish_grad, 0)

    @pl.when(sec == 0)
    def _():
        pl.semaphore_wait(wrapped, 1)

    relay_grad = start_remote(z_out.at[0], pass_grad, z_send.at[0], z_recv.at[0], before)

    operands = {OUT: (act_t, xc), IN: (dpre_t, nb)}
    size = hid // pieces
    bands = [pl.ds(p * size, size) for p in range(pieces)]
    sent = {}

    def product(g, p, owner):
        left, right = operands[g]
        return jnp.dot(
            left[bands[p], :], right[:, column(owner)], preferred_element_type=jnp.float32
        )

    def give(g):
        for p in range(pieces):
            if g == IN:
                backward_slope(far, p * size, size)
            parts[g, bands[p], :] = product(g, p, partner).astype(jnp.bfloat16)
            sent[g, p] = start_remote(
                parts.at[g, bands[p]], landed.at[g, bands[p]],
                rs_send.at[g, p], rs_recv.at[g, p], {"dp": partner},
            )

    def keep(g):
        for p in range(pieces):
            own_sum[g, bands[p], :] = product(g, p, dp)

    await_gather(0)
    normalise(xs, nb, tokens, tokens)
    backward_pre(far)
    await_gather(1)
    give(OUT)
    await_gather(2)
    keep(OUT)
    await_gather(3)
    await_gather(4)
    give(IN)
    keep(IN)

    for copy in [swap_fwd, swap_stash, swap_cot, *gathers, swap_grad, swap_branch]:
        copy.wait_send()
    for g, result in ((OUT, gout_ref), (IN, gin_ref)):
        for p in range(pieces):
            if (g, p) == (IN, pieces - 1):
                for copy in (relay_grad, relay_fwd):
                    copy.wait()
            sent[g, p].wait()
            result[bands[p], :] = (
                own_sum[g, bands[p], :] + landed[g, bands[p], :].astype(jnp.float32)
            ).astype(jnp.bfloat16)

def relay_on_device(fwd_in, stash, cot, w_in, w_out, gain):
    rows, width = stash.shape[1:]
    hid = w_in.shape[1]
    tokens = rows * lax.axis_size("mp")
    cols = width // lax.axis_size("dp")
    bf16 = jnp.bfloat16
    vmem = pl.BlockSpec(memory_space=pltpu.VMEM)
    hbm = pl.BlockSpec(memory_space=pl.ANY)
    dma = pltpu.SemaphoreType.DMA
    held = (rows * width + hid * cols) * 2 * jnp.dtype(bf16).itemsize
    results = pl.pallas_call(
        relay_kernel,
        out_shape=(pltpu.VMEM((rows, width), bf16),) * 2 + (pltpu.VMEM((hid, cols), bf16),) * 2,
        in_specs=[hbm] * 6,
        out_specs=(vmem,) * 4,
        scratch_shapes=[
            pltpu.VMEM((1, width), jnp.float32),
            pltpu.VMEM((tokens, width), bf16),
            pltpu.VMEM((2 * tokens, width), bf16),
            pltpu.VMEM((2 * tokens, width), bf16),
            pltpu.VMEM((hid, width), bf16),
            pltpu.VMEM((hid, width), bf16),
            pltpu.VMEM((tokens, width), bf16),
            pltpu.VMEM((2 * tokens, width), bf16),
            pltpu.VMEM((hid, tokens), jnp.float32),
            pltpu.VMEM((hid, 2 * tokens), bf16),
            pltpu.VMEM((hid, 2 * tokens), bf16),
            pltpu.VMEM((rows, hid), bf16),
            pltpu.VMEM((2, hid, cols), jnp.float32),
            pltpu.VMEM((2, hid, cols), bf16),
            pltpu.VMEM((2, hid, cols), bf16),
            pltpu.VMEM((2, rows, width), bf16),
            pltpu.VMEM((2, rows, width), bf16),
            pltpu.VMEM((2, rows, width), bf16),
            pltpu.VMEM((2, rows, width), bf16),
            dma((6,)),
            dma((3,)),
            dma((3,)),
            dma((2, 5)),
            dma((2, 5)),
            dma((2,)),
            dma((2,)),
            dma((2, pieces)),
            dma((2, pieces)),
            dma((2,)),
            dma((2,)),
            *[pltpu.SemaphoreType.REGULAR] * 3,
            pltpu.SemaphoreType.REGULAR((3,)),
        ],
        compiler_params=pltpu.CompilerParams(
            collective_id=0, has_side_effects=True,
            vmem_limit_bytes=vmem_bytes - held - 2**17,
        ),
    )(fwd_in[0], stash[0], cot[0], w_in[0], w_out[0], gain)
    results = pl.pallas_call(
        write_kernel,
        out_shape=tuple(jax.ShapeDtypeStruct(r.shape, r.dtype) for r in results),
        in_specs=[vmem] * 4,
        out_specs=(hbm,) * 4,
        scratch_shapes=[dma((4,))],
        compiler_params=pltpu.CompilerParams(vmem_limit_bytes=4 * 2**20),
    )(*results)
    return tuple(r[None] for r in results)

def fits_relay(mesh):
    return mesh.shape["dp"] == 4 and mesh.shape["mp"] == 2 and mesh.shape["section"] > 1

def solution(mesh):
    in_specs = (
        P("section", ("dp", "mp"), None),
        P("section", ("dp", "mp"), None),
        P("section", ("dp", "mp"), None),
        P("section", "mp", None),
        P("section", "mp", None),
        P("section", None),
    )
    out_specs = (
        P("section", ("dp", "mp"), None),
        P("section", ("dp", "mp"), None),
        P("section", "mp", "dp"),
        P("section", "mp", "dp"),
    )
    return jax.shard_map(
        relay_on_device if fits_relay(mesh) else on_device,
        mesh=mesh,
        in_specs=in_specs,
        out_specs=out_specs,
        check_vma=False,
    )
```

```python
import jax
import jax.numpy as jnp
from jax import lax
from jax.experimental import pallas as pl
from jax.experimental.pallas import tpu as pltpu
from jax.sharding import PartitionSpec as P

norm_eps = 1e-05
gelu_coef = 0.7978845608

def shifted(x, axis, by):
    length = lax.axis_size(axis)
    return lax.ppermute(x, axis, [(i, (i + by) % length) for i in range(length)])

def gelu_value(v):
    inner = jnp.tanh(gelu_coef * (v + 0.044715 * v * v * v))
    return 0.5 * v * (1.0 + inner)

def gelu_slope(v):
    inner = jnp.tanh(gelu_coef * (v + 0.044715 * v * v * v))
    return 0.5 * (1.0 + inner) + 0.5 * v * (1.0 - inner * inner) * gelu_coef * (
        1.0 + 0.134145 * v * v
    )

def prepare(x, w_first, gain_row):
    xf = x.astype(jnp.float32)
    scale = lax.rsqrt(jnp.mean(xf * xf, axis=-1, keepdims=True) + norm_eps)
    normed = (xf * scale * gain_row[None, :]).astype(jnp.bfloat16)
    pre = lax.dot_general(
        normed, w_first, (((1,), (1,)), ((), ())), preferred_element_type=jnp.float32
    )
    act = gelu_value(pre).astype(jnp.bfloat16)
    return (scale, normed, pre, act)

def on_device(fwd_in, stash, cot, w_in, w_out, gain):
    x_fwd = fwd_in[0]
    x_bwd = stash[0]
    cot_local = cot[0]
    w_first = w_in[0]
    w_second = w_out[0]
    gain_row = gain[0]
    local_rows = x_fwd.shape[0]
    scale, normed, pre, act = prepare(
        lax.all_gather(x_fwd, "mp", axis=0, tiled=True), w_first, gain_row
    )
    terms = jnp.dot(act, w_second, preferred_element_type=jnp.float32)
    branch = lax.psum_scatter(
        terms.astype(jnp.bfloat16), "mp", scatter_dimension=0, tiled=True
    ).astype(jnp.float32)
    out = (x_fwd.astype(jnp.float32) + branch).astype(jnp.bfloat16)
    passed_fwd = shifted(out, "section", 1)
    rows_x, rows_cot = (
        lax.all_gather(x_bwd, "mp", axis=0, tiled=True),
        lax.all_gather(cot_local, "mp", axis=0, tiled=True),
    )
    scale, normed, pre, act = prepare(rows_x, w_first, gain_row)
    d_act = lax.dot_general(
        rows_cot, w_second, (((1,), (1,)), ((), ())), preferred_element_type=jnp.float32
    )
    d_pre = (d_act * gelu_slope(pre)).astype(jnp.bfloat16)
    d_norm = lax.psum_scatter(
        jnp.dot(d_pre, w_first, preferred_element_type=jnp.float32).astype(jnp.bfloat16),
        "mp",
        scatter_dimension=0,
        tiled=True,
    ).astype(jnp.float32)
    offset = lax.axis_index("mp") * local_rows
    own_scale = lax.dynamic_slice_in_dim(scale, offset, local_rows, 0)
    shard_x = x_bwd.astype(jnp.float32)
    push = d_norm * gain_row[None, :]
    mixed = jnp.mean(shard_x * push, axis=-1, keepdims=True)
    dx = (
        cot_local.astype(jnp.float32)
        + own_scale * push
        - shard_x * own_scale * own_scale * own_scale * mixed
    )
    passed_grad = shifted(dx.astype(jnp.bfloat16), "section", -1)
    term_out = lax.dot_general(
        act, rows_cot, (((0,), (0,)), ((), ())), preferred_element_type=jnp.float32
    )
    term_in = lax.dot_general(
        d_pre, normed, (((0,), (0,)), ((), ())), preferred_element_type=jnp.float32
    )
    sum_in, sum_out = (
        lax.psum_scatter(
            term_in.astype(jnp.bfloat16), "dp", scatter_dimension=1, tiled=True
        ).astype(jnp.float32),
        lax.psum_scatter(
            term_out.astype(jnp.bfloat16), "dp", scatter_dimension=1, tiled=True
        ).astype(jnp.float32),
    )
    return (
        passed_fwd[None],
        passed_grad[None],
        sum_in.astype(jnp.bfloat16)[None],
        sum_out.astype(jnp.bfloat16)[None],
    )

MESH = pl.DeviceIdType.MESH
vmem_bytes = 67_043_328
NT = (((1,), (1,)), ((), ()))
TN = (((0,), (0,)), ((), ()))
OUT, IN = range(2)
pieces = 4

def tile_of(total, most):
    size = min(total, most)
    while total % size:
        size //= 2
    return size

def remote(src, dst, send, recv, target):
    return pltpu.make_async_remote_copy(
        src_ref=src, dst_ref=dst, send_sem=send, recv_sem=recv,
        device_id=target, device_id_type=MESH,
    )

def start_remote(src, dst, send, recv, target):
    copy = remote(src, dst, send, recv, target)
    copy.start()
    return copy

def write_kernel(a, b, c, d, a_out, b_out, c_out, d_out, sems):
    copies = [
        pltpu.make_async_copy(src, dst, sems.at[i])
        for i, (src, dst) in enumerate(((a, a_out), (b, b_out), (c, c_out), (d, d_out)))
    ]
    for copy in copies:
        copy.start()
    for copy in copies:
        copy.wait()

def relay_kernel(
    fwd_hbm, stash_hbm, cot_hbm, win_hbm, wout_hbm, gain_hbm,
    pass_fwd, pass_grad, gin_ref, gout_ref,
    gain_ref, xf, xs, xc, win, wout,
    nf, nb, slope, act_t, dpre_t, act, own_sum, parts, landed,
    mp_out, mp_in, own_terms, z_out,
    load_sem, swap_send, swap_recv, ag_send, ag_recv,
    mp_send, mp_recv, rs_send, rs_recv, z_send, z_recv, above, below, wrapped, entered,
):
    rows = pass_fwd.shape[0]
    tokens = 2 * rows
    hid, width = win.shape
    cols = gin_ref.shape[1]
    n_sec = lax.axis_size("section")
    sec, dp, mp = lax.axis_index("section"), lax.axis_index("dp"), lax.axis_index("mp")
    y, x = lax.div(dp, 2), lax.rem(dp, 2)
    flip_x, flip_y = y * 2 + (1 - x), (1 - y) * 2 + x
    across = (1 - y) * 2 + (1 - x)
    peer = {"mp": 1 - mp}
    after, before = {"section": lax.rem(sec + 1, n_sec)}, {"section": lax.rem(sec + n_sec - 1, n_sec)}
    partner = mp * flip_y + (1 - mp) * flip_x

    barrier = pltpu.get_barrier_semaphore()
    beside = [[{"dp": chip, "mp": core} for core in (mp, 1 - mp)] for chip in (flip_x, flip_y)]

    def signal(sem, target):
        pl.semaphore_signal(sem, inc=1, device_id=target, device_id_type=MESH)

    @pl.when(mp == 1)
    def _():
        signal(barrier, peer)

    for low, targets in zip((x == 0, y == 0), beside):
        @pl.when(low)
        def _(targets=targets):
            for target in targets:
                signal(barrier, target)

    @pl.when(sec < n_sec - 1)
    def _():
        signal(barrier, after)

    own, other = pl.ds(0, rows), pl.ds(rows, rows)
    near, far = pl.ds(0, tokens), pl.ds(tokens, tokens)
    local = (
        (stash_hbm, xs.at[own]), (cot_hbm, xc.at[own]), (fwd_hbm, xf.at[own]),
        (gain_hbm, gain_ref), (win_hbm, win), (wout_hbm, wout),
    )
    loads = [
        pltpu.make_async_copy(src, dst, load_sem.at[i]) for i, (src, dst) in enumerate(local)
    ]
    load_stash, load_cot, load_fwd, load_gain, load_win, load_wout = loads
    awaited = 1 - mp + 2 * x + 2 * y + jnp.minimum(sec, 1)

    @pl.when(awaited > 0)
    def _():
        pl.semaphore_wait(barrier, awaited)

    def column(block):
        return pl.ds(pl.multiple_of(block * cols, cols), cols)

    targets = (
        ({"dp": flip_x, "mp": 1}, (across, flip_x, dp, flip_y)),
        ({"dp": flip_y, "mp": 0}, (across, flip_y, dp, flip_x)),
    )
    slot = pl.ds(pl.multiple_of(tokens + mp * rows, rows), rows)
    gathers = []
    for d, (target, _) in enumerate(targets):
        gathers.append(
            remote(stash_hbm, xs.at[slot], ag_send.at[d, 0], ag_recv.at[mp, 0], target)
        )
    for d, copy in enumerate(gathers):
        @pl.when((x, y)[d] == 1)
        def _(copy=copy):
            copy.start()

    @pl.when(mp == 0)
    def _():
        signal(entered.at[2], peer)

    for i, (high, cores) in enumerate(zip((x == 1, y == 1), beside)):
        @pl.when(high)
        def _(i=i, cores=cores):
            for target in cores:
                signal(entered.at[i], target)

    for load in loads:
        load.start()

    for d, copy in enumerate(gathers):
        @pl.when((x, y)[d] == 0)
        def _(d=d, copy=copy):
            pl.semaphore_wait(entered.at[d], 2)
            copy.start()

    for i in range(4):
        for d, (target, order) in enumerate(targets):
            at = column(order[i])
            gathers.append(
                start_remote(
                    cot_hbm.at[:, at], xc.at[slot, at],
                    ag_send.at[d, 1 + i], ag_recv.at[mp, 1 + i], target,
                )
            )

    @pl.when(mp == 1)
    def _():
        pl.semaphore_wait(entered.at[2], 1)

    load_fwd.wait()
    swap_fwd = start_remote(xf.at[own], xf.at[other], swap_send.at[0], swap_recv.at[0], peer)
    load_stash.wait()
    load_cot.wait()
    swap_stash = start_remote(xs.at[own], xs.at[other], swap_send.at[1], swap_recv.at[1], peer)
    swap_cot = start_remote(xc.at[own], xc.at[other], swap_send.at[2], swap_recv.at[2], peer)
    @pl.when(sec > 0)
    def _():
        signal(above, before)

    @pl.when((sec == 1) & (sec < n_sec - 1))
    def _():
        pl.semaphore_wait(above, 1)
        signal(below, after)

    gathered = (partner, dp, (1 - mp) * flip_y + mp * flip_x, across)

    def await_gather(i):
        for core in range(2):
            rows_at = pl.ds(tokens + core * rows, rows)
            if i == 0:
                src, dst = xs.at[own], xs.at[rows_at]
            else:
                at = column(gathered[i - 1])
                src, dst = xc.at[own, at], xc.at[rows_at, at]
            remote(src, dst, ag_send.at[0, i], ag_recv.at[core, i], peer).wait_recv()

    step = tile_of(rows, 64)

    def normalise(source, target, first, count):
        def body(i, carry):
            at = pl.ds(pl.multiple_of(first + i * step, step), step)
            v = source[at, :].astype(jnp.float32)
            r = lax.rsqrt(jnp.mean(v * v, axis=-1, keepdims=True) + norm_eps)
            target[at, :] = (v * r * gain_ref[...]).astype(jnp.bfloat16)
            return carry

        lax.fori_loop(0, count // step, body, 0)

    block = tile_of(hid, 256)

    def backward_pre(span):
        def body(i, carry):
            at = pl.ds(pl.multiple_of(i * block, block), block)
            v = lax.dot_general(
                win[at, :], nb[span, :], NT, preferred_element_type=jnp.float32
            )
            square = v * v
            t = jnp.tanh(gelu_coef * (v + 0.044715 * square * v))
            act_t[at, span] = (0.5 * v * (1.0 + t)).astype(jnp.bfloat16)
            slope[at, :] = 0.5 * (1.0 + t) + 0.5 * v * (1.0 - t * t) * gelu_coef * (
                1.0 + 0.134145 * square
            )
            return carry

        lax.fori_loop(0, hid // block, body, 0)

    def backward_slope(span, first, count):
        size = tile_of(count, 256)

        def body(i, carry):
            at = pl.ds(pl.multiple_of(first + i * size, size), size)
            d_act = lax.dot_general(
                wout[at, :], xc[span, :], NT, preferred_element_type=jnp.float32
            )
            dpre_t[at, span] = (d_act * slope[at, :]).astype(jnp.bfloat16)
            return carry

        lax.fori_loop(0, count // size, body, 0)

    def forward(span):
        def body(i, carry):
            at = pl.ds(pl.multiple_of(i * block, block), block)
            v = lax.dot_general(
                nf[span, :], win[at, :], NT, preferred_element_type=jnp.float32
            )
            t = jnp.tanh(gelu_coef * (v + 0.044715 * v * v * v))
            act[:, at] = (0.5 * v * (1.0 + t)).astype(jnp.bfloat16)
            return carry

        lax.fori_loop(0, hid // block, body, 0)
        return jnp.dot(
            act[...], wout[...], preferred_element_type=jnp.float32
        ).astype(jnp.bfloat16)

    load_gain.wait()
    normalise(xf, nf, 0, rows)
    load_win.wait()
    load_wout.wait()
    swap_fwd.wait_recv()
    normalise(xf, nf, rows, rows)
    mp_out[1] = forward(other)
    swap_branch = start_remote(mp_out.at[1], mp_in.at[1], mp_send.at[1], mp_recv.at[1], peer)

    @pl.when((sec > 1) & (sec < n_sec - 1))
    def _():
        pl.semaphore_wait(above, 1)
        pl.semaphore_wait(below, 1)
        signal(below, after)

    own_terms[1] = forward(own)
    swap_branch.wait_recv()

    def finish_forward(i, carry):
        at = pl.ds(pl.multiple_of(i * step, step), step)
        branch = own_terms[1, at, :].astype(jnp.float32) + mp_in[1, at, :].astype(jnp.float32)
        z_out[1, at, :] = (xf[at, :].astype(jnp.float32) + branch).astype(jnp.bfloat16)
        return carry

    lax.fori_loop(0, rows // step, finish_forward, 0)

    @pl.when(sec == 0)
    def _():
        pl.semaphore_wait(above, 1)

    if n_sec > 2:
        @pl.when(sec == n_sec - 1)
        def _():
            pl.semaphore_wait(below, 1)

    @pl.when(sec == n_sec - 1)
    def _():
        signal(wrapped, after)

    relay_fwd = start_remote(z_out.at[1], pass_fwd, z_send.at[1], z_recv.at[1], after)

    swap_stash.wait_recv()
    normalise(xs, nb, 0, tokens)
    backward_pre(near)
    swap_cot.wait_recv()
    backward_slope(near, 0, hid)

    def d_norm(span):
        return lax.dot_general(
            dpre_t[:, span], win[...], TN, preferred_element_type=jnp.float32
        ).astype(jnp.bfloat16)

    mp_out[0] = d_norm(other)
    swap_grad = start_remote(mp_out.at[0], mp_in.at[0], mp_send.at[0], mp_recv.at[0], peer)
    own_terms[0] = d_norm(own)
    swap_grad.wait_recv()

    def finish_grad(i, carry):
        at = pl.ds(pl.multiple_of(i * step, step), step)
        v = xs[at, :].astype(jnp.float32)
        r = lax.rsqrt(jnp.mean(v * v, axis=-1, keepdims=True) + norm_eps)
        push = (
            own_terms[0, at, :].astype(jnp.float32) + mp_in[0, at, :].astype(jnp.float32)
        ) * gain_ref[...]
        mixed = jnp.mean(v * push, axis=-1, keepdims=True)
        dx = xc[at, :].astype(jnp.float32) + r * push - v * (r * r * r * mixed)
        z_out[0, at, :] = dx.astype(jnp.bfloat16)
        return carry

    lax.fori_loop(0, rows // step, finish_grad, 0)

    @pl.when(sec == 0)
    def _():
        pl.semaphore_wait(wrapped, 1)

    relay_grad = start_remote(z_out.at[0], pass_grad, z_send.at[0], z_recv.at[0], before)

    operands = {OUT: (act_t, xc), IN: (dpre_t, nb)}
    size = hid // pieces
    bands = [pl.ds(p * size, size) for p in range(pieces)]
    sent = {}

    def product(g, p, owner):
        left, right = operands[g]
        return jnp.dot(
            left[bands[p], :], right[:, column(owner)], preferred_element_type=jnp.float32
        )

    def give(g):
        for p in range(pieces):
            if g == IN:
                backward_slope(far, p * size, size)
            parts[g, bands[p], :] = product(g, p, partner).astype(jnp.bfloat16)
            sent[g, p] = start_remote(
                parts.at[g, bands[p]], landed.at[g, bands[p]],
                rs_send.at[g, p], rs_recv.at[g, p], {"dp": partner},
            )

    def keep(g):
        for p in range(pieces):
            own_sum[g, bands[p], :] = product(g, p, dp)

    await_gather(0)
    normalise(xs, nb, tokens, tokens)
    backward_pre(far)
    await_gather(1)
    give(OUT)
    await_gather(2)
    keep(OUT)
    await_gather(3)
    await_gather(4)
    give(IN)
    keep(IN)

    for copy in [swap_fwd, swap_stash, swap_cot, *gathers, swap_grad, swap_branch]:
        copy.wait_send()
    for g, result in ((OUT, gout_ref), (IN, gin_ref)):
        for p in range(pieces):
            if (g, p) == (IN, pieces - 1):
                for copy in (relay_grad, relay_fwd):
                    copy.wait()
            sent[g, p].wait()
            result[bands[p], :] = (
                own_sum[g, bands[p], :] + landed[g, bands[p], :].astype(jnp.float32)
            ).astype(jnp.bfloat16)

def relay_on_device(fwd_in, stash, cot, w_in, w_out, gain):
    rows, width = stash.shape[1:]
    hid = w_in.shape[1]
    tokens = rows * lax.axis_size("mp")
    cols = width // lax.axis_size("dp")
    bf16 = jnp.bfloat16
    vmem = pl.BlockSpec(memory_space=pltpu.VMEM)
    hbm = pl.BlockSpec(memory_space=pl.ANY)
    dma = pltpu.SemaphoreType.DMA
    held = (rows * width + hid * cols) * 2 * jnp.dtype(bf16).itemsize
    results = pl.pallas_call(
        relay_kernel,
        out_shape=(pltpu.VMEM((rows, width), bf16),) * 2 + (pltpu.VMEM((hid, cols), bf16),) * 2,
        in_specs=[hbm] * 6,
        out_specs=(vmem,) * 4,
        scratch_shapes=[
            pltpu.VMEM((1, width), jnp.float32),
            pltpu.VMEM((tokens, width), bf16),
            pltpu.VMEM((2 * tokens, width), bf16),
            pltpu.VMEM((2 * tokens, width), bf16),
            pltpu.VMEM((hid, width), bf16),
            pltpu.VMEM((hid, width), bf16),
            pltpu.VMEM((tokens, width), bf16),
            pltpu.VMEM((2 * tokens, width), bf16),
            pltpu.VMEM((hid, tokens), jnp.float32),
            pltpu.VMEM((hid, 2 * tokens), bf16),
            pltpu.VMEM((hid, 2 * tokens), bf16),
            pltpu.VMEM((rows, hid), bf16),
            pltpu.VMEM((2, hid, cols), jnp.float32),
            pltpu.VMEM((2, hid, cols), bf16),
            pltpu.VMEM((2, hid, cols), bf16),
            pltpu.VMEM((2, rows, width), bf16),
            pltpu.VMEM((2, rows, width), bf16),
            pltpu.VMEM((2, rows, width), bf16),
            pltpu.VMEM((2, rows, width), bf16),
            dma((6,)),
            dma((3,)),
            dma((3,)),
            dma((2, 5)),
            dma((2, 5)),
            dma((2,)),
            dma((2,)),
            dma((2, pieces)),
            dma((2, pieces)),
            dma((2,)),
            dma((2,)),
            *[pltpu.SemaphoreType.REGULAR] * 3,
            pltpu.SemaphoreType.REGULAR((3,)),
        ],
        compiler_params=pltpu.CompilerParams(
            collective_id=0, has_side_effects=True,
            vmem_limit_bytes=vmem_bytes - held - 2**17,
        ),
    )(fwd_in[0], stash[0], cot[0], w_in[0], w_out[0], gain)
    results = pl.pallas_call(
        write_kernel,
        out_shape=tuple(jax.ShapeDtypeStruct(r.shape, r.dtype) for r in results),
        in_specs=[vmem] * 4,
        out_specs=(hbm,) * 4,
        scratch_shapes=[dma((4,))],
        compiler_params=pltpu.CompilerParams(vmem_limit_bytes=4 * 2**20),
    )(*results)
    return tuple(r[None] for r in results)

def fits_relay(mesh):
    return mesh.shape["dp"] == 4 and mesh.shape["mp"] == 2 and mesh.shape["section"] > 1

def solution(mesh):
    in_specs = (
        P("section", ("dp", "mp"), None),
        P("section", ("dp", "mp"), None),
        P("section", ("dp", "mp"), None),
        P("section", "mp", None),
        P("section", "mp", None),
        P("section", None),
    )
    out_specs = (
        P("section", ("dp", "mp"), None),
        P("section", ("dp", "mp"), None),
        P("section", "mp", "dp"),
        P("section", "mp", "dp"),
    )
    return jax.shard_map(
        relay_on_device if fits_relay(mesh) else on_device,
        mesh=mesh,
        in_specs=in_specs,
        out_specs=out_specs,
        check_vma=False,
    )
```
